32 devices in a mesh: band: 8 (over z, x), ens: 4 (over y, core).
Axes of the slice: x: 2, y: 2, z: 4, core: 2. Of those that a mesh axis runs over, the one named last changes fastest.
Arguments:
- grid_latent: bfloat16 [4, 1024, 1024], P('ens', 'band'), may hold values from -6 to 6
- hidden: bfloat16 [4, 256, 1024], P('ens', 'band'), may hold values from -6 to 6
- d_updated: bfloat16 [4, 256, 1024], P('ens', 'band'), may hold values from -6 to 6
- w_kv: bfloat16 [1024, 2048], replicated, may hold values from -0.1875 to 0.1875
- w_q: bfloat16 [1024, 1024], replicated, may hold values from -0.1875 to 0.1875
- src_gain: float32 [1024], replicated, may hold values from 0.1 to 1.9
- q_gain: float32 [1024], replicated, may hold values from 0.5 to 40
- src_index: int32 [256, 12], P('band'), may hold values from 0 to 1023, as said below
- edge_mask: int32 [256, 12], P('band'), may hold values from 0 to 1, as said below
Outputs:
- updated: bfloat16 [4, 256, 1024], P('ens', 'band')
- d_grid: bfloat16 [4, 1024, 1024], P('ens', 'band')
- d_wkv_t: float32 [2048, 1024], P(('band', 'ens'))
The draws below stay inside these ranges and needn't reach their ends.
Inputs may be any that keep to these rules, and one draw needn't show every extreme that they name: `src_index`: every edge slot of hidden node h names a grid row from max(0, (h // 32) * 128 - 32) to min(1024, (h // 32 + 1) * 128 + 32) - 1, and in every band both ends of that range are named by a valid edge. `edge_mask`: the first slot of every hidden node is valid.
All inputs are finite; a program needn't handle non-finite values.
Results may differ from the reference program's by a relative error of at most 0.013.
The reference program's roundings to bfloat16 on the way count: a program that leaves them out, or rounds other values in their place, can miss the bound.
Values may be sent and summed in bfloat16 or wider, within the bound.
No kernel may reach another device: no remote copies, remote signals or barrier semaphores. Data moves between devices by JAX's collectives and lax.ppermute only.
A program may use at most 128 MiB of HBM per device.

```python
import math
import jax
import jax.numpy as jnp
from jax import lax

D = 1024
HEADS = 16
K = 12
R = 32
G_DEV = 128
H_DEV = 32
MEMBERS = 4
G = 1024
H = 256
N_BAND = 8


def draw_q_gain(key, part):
    return jax.random.uniform(key, (D,), jnp.float32, 0.5, 1.5)


def draw_src_index(key, part):
    nodes = jnp.arange(H, dtype=jnp.int32)
    band_index = nodes // H_DEV
    lowest = jnp.maximum(band_index * G_DEV - R, 0)
    highest = jnp.minimum((band_index + 1) * G_DEV + R, G)
    picks = jax.random.randint(key, (H, K), lowest[:, None], highest[:, None], dtype=jnp.int32)
    within = nodes % H_DEV
    first_slot = jnp.where(within == 0, lowest, jnp.where(within == 1, highest - 1, picks[:, 0]))
    return picks.at[:, 0].set(first_slot)


def draw_edge_mask(key, part):
    levels = jax.random.randint(key, (H, K), 0, 4, dtype=jnp.int32)
    valid = (levels > 0).astype(jnp.int32)
    return valid.at[:, 0].set(1)


def block_scale(own_key, dims, cuts, least, top_value):
    gain, own = 1.0, jax.random.fold_in(own_key, 6)
    for position, blocks in cuts:
        draws = jnp.exp(jax.random.uniform(jax.random.fold_in(own, position), (blocks,), jnp.float32, least / len(cuts), top_value / len(cuts)))
        gain = gain * jnp.repeat(draws, dims[position] // blocks).reshape([-1 if axis == position else 1 for axis in range(len(dims))])
    return gain


def scatter_about(key, extent, deviation, limit, pieces=(), held_as=jnp.bfloat16):
    drawn = jax.random.normal(key, extent, jnp.float32) * deviation
    if len(pieces) > 0:
        drawn = block_scale(key, extent, pieces, -0.22, 0.18) * drawn
    return jnp.clip(drawn, min=-limit, max=limit).astype(held_as)


def setup_inputs(seed: int = 0) -> dict:
    streams_of = jax.random.split(jax.random.key(seed), 10)
    return {
        "grid_latent": scatter_about(streams_of[0], (MEMBERS, G, D), 1.0, 6.0, ((0, 4), (1, 8))),
        "hidden": scatter_about(streams_of[1], (MEMBERS, H, D), 1.0, 6.0, ((0, 4), (1, 8))),
        "d_updated": scatter_about(streams_of[2], (MEMBERS, H, D), 1.0, 6.0, ((0, 4), (1, 8))),
        "w_kv": scatter_about(streams_of[3], (D, 2 * D), D ** -0.5, 0.1875),
        "w_q": scatter_about(streams_of[4], (D, D), D ** -0.5, 0.1875),
        "src_gain": jnp.clip(1.0 + 0.18 * jax.random.normal(streams_of[5], (D,), jnp.float32), 0.1, 1.9),
        "q_gain": draw_q_gain(jax.random.fold_in(streams_of[9], 71), 0),
        "src_index": draw_src_index(jax.random.fold_in(streams_of[9], 71), 0),
        "edge_mask": draw_edge_mask(jax.random.fold_in(streams_of[9], 71), 0),
    }


EPSILON = 1e-05

def normalize(values):
    values = values.astype(jnp.float32)
    average = lax.optimization_barrier(jnp.mean(values, axis=-1, keepdims=True))
    centred = values - average
    variance = lax.optimization_barrier(jnp.mean(centred * centred, axis=-1, keepdims=True))
    inv_std = lax.rsqrt(variance + EPSILON)
    return (centred * inv_std, inv_std)

def times_transposed(left, right):
    return lax.dot_general(left, right, (((1,), (1,)), ((), ())), preferred_element_type=jnp.float32)

def node_block(queries, hidden_rows, cotangent, kv_window, local_rows, valid_edges):
    node_count, features = queries.shape
    head_dim = features // HEADS
    score_scale = 1.0 / math.sqrt(head_dim)
    highest = lax.Precision.HIGHEST
    gathered = kv_window[local_rows]
    key_rows = gathered[..., :features].reshape(node_count, K, HEADS, head_dim).astype(jnp.float32)
    value_rows = gathered[..., features:].reshape(node_count, K, HEADS, head_dim).astype(jnp.float32)
    query_heads = queries.reshape(node_count, HEADS, head_dim).astype(jnp.float32)
    scores = jnp.einsum('hnd,hknd->hkn', query_heads, key_rows, precision=highest) * score_scale
    valid = valid_edges[:, :, None] > 0
    shifted = jnp.where(valid, scores, -jnp.inf)
    row_max = lax.optimization_barrier(jnp.max(shifted, axis=1, keepdims=True))
    exp_terms = jnp.exp(shifted - row_max)
    attn_probs = exp_terms / lax.optimization_barrier(jnp.sum(exp_terms, axis=1, keepdims=True))
    probs_low = attn_probs.astype(jnp.bfloat16)
    probs_wide = probs_low.astype(jnp.float32)
    attended = jnp.einsum('hkn,hknd->hnd', probs_wide, value_rows, precision=highest)
    attended = attended.reshape(node_count, features)
    updated = (hidden_rows.astype(jnp.float32) + attended).astype(jnp.bfloat16)
    d_wide = cotangent.astype(jnp.float32).reshape(node_count, HEADS, head_dim)
    d_probs = jnp.einsum('hnd,hknd->hkn', d_wide, value_rows, precision=highest)
    d_scores = attn_probs * (d_probs - lax.optimization_barrier(jnp.sum(attn_probs * d_probs, axis=1, keepdims=True)))
    d_keys = d_scores[..., None] * query_heads[:, None] * score_scale
    d_values = probs_wide[..., None] * d_wide[:, None]
    edge_grads = jnp.concatenate([d_keys.reshape(node_count * K, features), d_values.reshape(node_count * K, features)], axis=1)
    partial_value = jnp.zeros((kv_window.shape[0], 2 * features), jnp.float32).at[local_rows.reshape(-1)].add(edge_grads)
    return (updated, partial_value.astype(jnp.bfloat16))

def reference(grid_latent, hidden, d_updated, w_kv, w_q, src_gain, q_gain, src_index, edge_mask):
    features = w_q.shape[0]
    standard, inv_std = normalize(grid_latent)
    gain_wide = src_gain.astype(jnp.float32)
    normed = (standard * gain_wide).astype(jnp.bfloat16)
    kv_all = jnp.dot(normed.reshape(MEMBERS * G, features), w_kv, preferred_element_type=jnp.float32)
    kv_all = kv_all.astype(jnp.bfloat16).reshape(MEMBERS, G, 2 * features)
    kv_padded = jnp.pad(kv_all, ((0, 0), (R, R), (0, 0)))
    normed_padded = jnp.pad(normed, ((0, 0), (R, R), (0, 0)))
    hidden_hat, _ = normalize(hidden)
    hidden_normed = (hidden_hat * q_gain.astype(jnp.float32)).astype(jnp.bfloat16)
    queries = jnp.dot(hidden_normed.reshape(MEMBERS * H, features), w_q, preferred_element_type=jnp.float32)
    queries = queries.astype(jnp.bfloat16).reshape(MEMBERS, H, features)
    window = G_DEV + 2 * R
    zero_index = jnp.zeros((), jnp.int32)

    def one_band(carry, step_index):
        d_padded, d_weights = carry
        member = (step_index // N_BAND).astype(jnp.int32)
        band_index = (step_index % N_BAND).astype(jnp.int32)
        first_row = (band_index * G_DEV).astype(jnp.int32)
        first_node = (band_index * H_DEV).astype(jnp.int32)
        kv_window = lax.dynamic_slice(kv_padded, (member, first_row, zero_index), (1, window, 2 * features))[0]
        normed_window = lax.dynamic_slice(normed_padded, (member, first_row, zero_index), (1, window, features))[0]
        query_rows = lax.dynamic_slice(queries, (member, first_node, zero_index), (1, H_DEV, features))[0]
        hidden_rows = lax.dynamic_slice(hidden, (member, first_node, zero_index), (1, H_DEV, features))[0]
        cotangent = lax.dynamic_slice(d_updated, (member, first_node, zero_index), (1, H_DEV, features))[0]
        local_rows = (lax.dynamic_slice(src_index, (first_node, zero_index), (H_DEV, K)) - (first_row - R)).astype(jnp.int32)
        valid_edges = lax.dynamic_slice(edge_mask, (first_node, zero_index), (H_DEV, K))
        updated_rows, partial_value = node_block(query_rows, hidden_rows, cotangent, kv_window, local_rows, valid_edges)
        d_window = times_transposed(partial_value, w_kv)
        current = lax.dynamic_slice(d_padded, (member, first_row, zero_index), (1, window, features))
        d_padded = lax.dynamic_update_slice(d_padded, current + d_window[None], (member, first_row, zero_index))
        d_weights = d_weights + lax.dot_general(partial_value, normed_window, (((0,), (0,)), ((), ())), preferred_element_type=jnp.float32)
        return ((d_padded, d_weights), updated_rows)
    start_carry = (jnp.zeros((MEMBERS, G + 2 * R, features), jnp.float32), jnp.zeros((2 * features, features), jnp.float32))
    (d_padded, d_weights), updated = lax.scan(one_band, start_carry, jnp.arange(MEMBERS * N_BAND, dtype=jnp.int32))
    updated = updated.reshape(MEMBERS, H, features)
    d_normed = d_padded[:, R:R + G]
    d_scaled = d_normed * gain_wide
    d_grid = inv_std * (d_scaled - lax.optimization_barrier(jnp.mean(d_scaled, axis=-1, keepdims=True)) - standard * lax.optimization_barrier(jnp.mean(d_scaled * standard, axis=-1, keepdims=True)))
    d_wkv_t = d_weights * (1.0 / math.sqrt(MEMBERS * G))
    return (updated, d_grid.astype(jnp.bfloat16), d_wkv_t)
```

```python
import functools
import math

import jax
import jax.numpy as jnp
from jax import lax
from jax.experimental import pallas as pl
from jax.experimental.pallas import tpu as pltpu
from jax.sharding import PartitionSpec as P

HEADS = 16
K = 12
R = 32
EPSILON = 1e-05
F32 = jnp.float32
BF16 = jnp.bfloat16


def spec(space=pltpu.VMEM):
    return pl.BlockSpec(memory_space=space)


def estimate(flops, moved):
    return pl.CostEstimate(flops=int(flops), bytes_accessed=int(moved), transcendentals=0)


def dot(left, right):
    return jnp.dot(left, right, preferred_element_type=F32)


def dot_rows(left, right):
    return lax.dot_general(left, right, (((0,), (0,)), ((), ())), preferred_element_type=F32)


def dot_lanes(left, right):
    return lax.dot_general(left, right, (((1,), (1,)), ((), ())), preferred_element_type=F32)


def halves(wide):
    high = wide.astype(BF16)
    return high, (wide - high.astype(F32)).astype(BF16)


def normalize(values):
    values = values.astype(F32)
    average = jnp.mean(values, axis=-1, keepdims=True)
    centred = values - average
    variance = jnp.mean(centred * centred, axis=-1, keepdims=True)
    inv_std = lax.rsqrt(variance + EPSILON)
    return centred * inv_std, inv_std


def norm_kernel(grid_ref, gain_ref, normed_ref):
    standard, _ = normalize(grid_ref[...])
    normed_ref[...] = (standard * gain_ref[...]).astype(BF16)


def project_kernel(hidden_ref, gain_ref, wq_ref, normed_ref, wkv_ref, q_ref, kv_ref, hat_ref):
    @pl.when(pl.program_id(0) == 0)
    def _():
        standard, _ = normalize(hidden_ref[...])
        hat_ref[...] = (standard * gain_ref[...]).astype(BF16)

    q_ref[...] = dot(hat_ref[...], wq_ref[...]).astype(BF16)
    kv_ref[...] = dot(normed_ref[...], wkv_ref[...]).astype(BF16)


def attend_kernel(
    groups, block, where_ref, low_ref, high_ref, wkv_ref, kv_ref, q_ref, cot_ref, hidden_ref,
    index_ref, mask_ref, *refs
):
    updated_ref, partial_ref = refs[:2]
    piece_refs = refs[2:-2]
    window_ref, pieces_ref = refs[-2:]
    nodes, features = q_ref.shape
    own = kv_ref.shape[0]
    rows = own + 2 * R
    lanes = 128
    head_dim = features // HEADS
    shift = head_dim.bit_length() - 1
    scale = 1.0 / math.sqrt(head_dim)
    window_ref[:R] = dot(low_ref[...], wkv_ref[...]).astype(BF16)
    window_ref[R : R + own] = kv_ref[...]
    window_ref[R + own :] = dot(high_ref[...], wkv_ref[...]).astype(BF16)

    local = index_ref[...] - where_ref[0]
    row_id = lax.broadcasted_iota(jnp.int32, (nodes, rows), 1)
    picks = jnp.concatenate(
        [jnp.where(row_id == local[:, k : k + 1], 1.0, 0.0).astype(BF16) for k in range(K)], axis=0
    )
    valid = jnp.concatenate([mask_ref[:, k : k + 1] for k in range(K)], axis=0) > 0
    chunk = 256
    feature_id = lax.broadcasted_iota(jnp.int32, (features, lanes), 0)
    lane_id = lax.broadcasted_iota(jnp.int32, (features, lanes), 1)
    to_heads = jnp.where(jnp.right_shift(feature_id, shift) == lane_id, 1.0, 0.0).astype(BF16)
    lane_t = lax.broadcasted_iota(jnp.int32, (lanes, features), 0)
    feature_t = lax.broadcasted_iota(jnp.int32, (lanes, features), 1)
    from_heads = jnp.where(jnp.right_shift(feature_t, shift) == lane_t, 1.0, 0.0).astype(BF16)

    def repeated(ref, c):
        return jnp.broadcast_to(ref[:, c : c + chunk].astype(F32)[None], (K, nodes, chunk))

    def by_edge(ref, c, start):
        edge = dot(picks, window_ref[:, start + c : start + c + chunk])
        product = edge.reshape(K, nodes, chunk) * repeated(ref, c)
        first, second = halves(product.reshape(K * nodes, chunk))
        heads = to_heads[c : c + chunk]
        return dot(first, heads) + dot(second, heads)

    scores = by_edge(q_ref, 0, 0)
    d_probs = by_edge(cot_ref, 0, features)
    for c in range(chunk, features, chunk):
        scores = scores + by_edge(q_ref, c, 0)
        d_probs = d_probs + by_edge(cot_ref, c, features)
    scores = jnp.where(valid, scores * scale, -jnp.inf).reshape(K, nodes, lanes)
    d_probs = d_probs.reshape(K, nodes, lanes)
    terms = jnp.exp(scores - jnp.max(scores, axis=0, keepdims=True))
    probs = terms / jnp.sum(terms, axis=0, keepdims=True)
    probs_low = probs.reshape(K * nodes, lanes).astype(BF16)
    inner = jnp.sum(probs * d_probs, axis=0, keepdims=True)
    d_scores = (probs * (d_probs - inner)).reshape(K * nodes, lanes)
    d_first, d_second = halves(d_scores)

    for c in range(0, features, chunk):
        heads = from_heads[:, c : c + chunk]
        spread = dot(probs_low, heads).reshape(K, nodes, chunk)
        values = dot(picks, window_ref[:, features + c : features + c + chunk])
        attended = jnp.sum(spread * values.reshape(K, nodes, chunk), axis=0)
        updated_ref[:, c : c + chunk] = (
            hidden_ref[:, c : c + chunk].astype(F32) + attended
        ).astype(BF16)
        first, second = halves((spread * repeated(cot_ref, c)).reshape(K * nodes, chunk))
        partial_ref[:, features + c : features + c + chunk] = (
            dot_rows(picks, first) + dot_rows(picks, second)
        ).astype(BF16)
        spread = (dot(d_first, heads) + dot(d_second, heads)).reshape(K, nodes, chunk)
        keys = (spread * repeated(q_ref, c)).reshape(K * nodes, chunk) * scale
        first, second = halves(keys)
        partial_ref[:, c : c + chunk] = (
            dot_rows(picks, first) + dot_rows(picks, second)
        ).astype(BF16)

    if piece_refs:
        left = lax.broadcasted_iota(jnp.int32, (rows, lanes), 1) < block
        for g in range(groups):
            for i in range(2 * features // (groups * lanes)):
                at = (2 * i * groups + g) * block
                a = at // lanes * lanes
                b = (at + groups * block) // lanes * lanes
                one = partial_ref[:, a : a + lanes].astype(F32)
                two = partial_ref[:, b : b + lanes].astype(F32)
                if at % lanes == 0:
                    two = pltpu.roll(two, block, 1)
                else:
                    one = pltpu.roll(one, block, 1)
                pieces_ref[g, :, i * lanes : (i + 1) * lanes] = jnp.where(left, one, two).astype(BF16)
        for k, piece_ref in enumerate(piece_refs):
            piece_ref[...] = pieces_ref[where_ref[1] ^ k]


def window_kernel(partial_ref, wkv_ref, own_ref, low_ref, high_ref):
    wide = dot_lanes(partial_ref[...], wkv_ref[...])
    rows = wide.shape[0]
    low_ref[...] = wide[:R].astype(BF16)
    own_ref[...] = wide[R : rows - R]
    high_ref[...] = wide[rows - R :].astype(BF16)


def product_kernel(groups, factor, where_ref, *refs):
    left_refs, right_refs = refs[:groups], refs[groups : 2 * groups]
    out_refs, total_ref = refs[2 * groups : -1], refs[-1]
    total = dot_rows(left_refs[0][...], right_refs[0][...])
    for left_ref, right_ref in zip(left_refs[1:], right_refs[1:]):
        total = total + dot_rows(left_ref[...], right_ref[...])
    total_ref[...] = total * factor
    block = out_refs[0].shape[0]
    for k, out_ref in enumerate(out_refs):
        start = pl.multiple_of((where_ref[2] ^ k) * block, block)
        out_ref[...] = total_ref[pl.ds(start, block)].astype(out_ref.dtype)


def finish_kernel(grid_ref, gain_ref, own_ref, low_ref, high_ref, out_ref, wide_ref):
    rows = own_ref.shape[0]
    wide_ref[...] = own_ref[...]
    wide_ref[:R] = wide_ref[:R] + low_ref[...].astype(F32)
    wide_ref[rows - R :] = wide_ref[rows - R :] + high_ref[...].astype(F32)
    standard, inv_std = normalize(grid_ref[...])
    scaled = wide_ref[...] * gain_ref[...]
    out_ref[...] = (
        inv_std
        * (
            scaled
            - jnp.mean(scaled, axis=-1, keepdims=True)
            - standard * jnp.mean(scaled * standard, axis=-1, keepdims=True)
        )
    ).astype(BF16)


def total_kernel(*refs):
    total = refs[0][...]
    for ref in refs[1:-1]:
        total = total + ref[...].astype(F32)
    refs[-1][...] = total


def swapped(value, axis, by):
    count = lax.axis_size(axis)
    return lax.ppermute(value, axis, [(i, i ^ by) for i in range(count)])


def passed_along(value, axis, by):
    peers = lax.axis_size(axis)
    pairs = [(i, i + by) for i in range(peers) if 0 <= i + by < peers]
    return lax.ppermute(value, axis, pairs)


def is_power(count):
    return count & (count - 1) == 0


def per_device(grid_latent, hidden, d_updated, w_kv, w_q, src_gain, q_gain, src_index, edge_mask):
    grid_latent, hidden, d_updated = grid_latent[0], hidden[0], d_updated[0]
    rows, features = grid_latent.shape
    nodes = hidden.shape[0]
    bands, members = lax.axis_size("band"), lax.axis_size("ens")
    band, member = lax.axis_index("band"), lax.axis_index("ens")
    window = rows + 2 * R
    block = 2 * features // (bands * members)
    src_gain, q_gain = src_gain[None], q_gain[None]
    where = jnp.stack([band * rows - R, member, band]).astype(jnp.int32)
    grouped = is_power(members) and is_power(bands) and bands <= 8 and block == 64 and members % 2 == 0

    normed = pl.pallas_call(
        norm_kernel,
        out_shape=jax.ShapeDtypeStruct((rows, features), BF16),
        in_specs=[spec()] * 2,
        out_specs=spec(),
        cost_estimate=estimate(10 * rows * features, 4 * rows * features),
        name="norm",
    )(grid_latent, src_gain)
    low = passed_along(normed[rows - R :], "band", 1)
    high = passed_along(normed[:R], "band", -1)

    steps = 4
    wide_q, wide_kv = features // steps, 2 * features // steps
    queries, kv = pl.pallas_call(
        project_kernel,
        grid=(steps,),
        out_shape=(
            jax.ShapeDtypeStruct((nodes, features), BF16),
            jax.ShapeDtypeStruct((rows, 2 * features), BF16),
        ),
        in_specs=[
            pl.BlockSpec((nodes, features), lambda i: (0, 0)),
            pl.BlockSpec((1, features), lambda i: (0, 0)),
            pl.BlockSpec((features, wide_q), lambda i: (0, i)),
            pl.BlockSpec((rows, features), lambda i: (0, 0)),
            pl.BlockSpec((features, wide_kv), lambda i: (0, i)),
        ],
        out_specs=(
            pl.BlockSpec((nodes, wide_q), lambda i: (0, i)),
            pl.BlockSpec((rows, wide_kv), lambda i: (0, i)),
        ),
        scratch_shapes=[pltpu.VMEM((nodes, features), BF16)],
        cost_estimate=estimate(2 * (2 * rows + nodes) * features * features, 6 * features * features),
        name="project",
    )(hidden, q_gain, w_q, normed, w_kv)

    normed_window = jnp.concatenate([low, normed, high], axis=0)

    pieces = members if grouped else 0
    columns = 2 * features // members
    outs = pl.pallas_call(
        functools.partial(attend_kernel, members, block),
        out_shape=[
            jax.ShapeDtypeStruct((nodes, features), BF16),
            jax.ShapeDtypeStruct((window, 2 * features), BF16),
        ]
        + [jax.ShapeDtypeStruct((window, columns), BF16)] * pieces,
        in_specs=[spec(pltpu.SMEM)] + [spec()] * 9,
        out_specs=[spec()] * (2 + pieces),
        scratch_shapes=[
            pltpu.VMEM((window, 2 * features), BF16),
            pltpu.VMEM((members, window, columns), BF16),
        ],
        cost_estimate=estimate(3e9, 10 * features * features),
        name="attend",
    )(where, low, high, w_kv, kv, queries, d_updated, hidden, src_index, edge_mask)
    updated, partial_value = outs[:2]
    lefts = outs[2:]

    factor = 1.0 / math.sqrt(members * rows * bands)
    if grouped:
        lefts = [lefts[0]] + [swapped(lefts[k], "ens", k) for k in range(1, members)]
        rights = [normed_window] + [swapped(normed_window, "ens", k) for k in range(1, members)]

    d_own, d_low, d_high = pl.pallas_call(
        window_kernel,
        out_shape=(
            jax.ShapeDtypeStruct((rows, features), F32),
            jax.ShapeDtypeStruct((R, features), BF16),
            jax.ShapeDtypeStruct((R, features), BF16),
        ),
        in_specs=[spec()] * 2,
        out_specs=(spec(),) * 3,
        cost_estimate=estimate(4 * window * features * features, 6 * features * features),
        name="window",
    )(partial_value, w_kv)
    back_high = passed_along(d_low, "band", -1)
    back_low = passed_along(d_high, "band", 1)

    if grouped:
        parts = pl.pallas_call(
            functools.partial(product_kernel, members, factor),
            out_shape=[jax.ShapeDtypeStruct((block, features), F32)]
            + [jax.ShapeDtypeStruct((block, features), BF16)] * (bands - 1),
            in_specs=[spec(pltpu.SMEM)] + [spec()] * (2 * members),
            out_specs=[spec()] * bands,
            scratch_shapes=[pltpu.VMEM((columns, features), F32)],
            cost_estimate=estimate(2 * members * window * columns * features, 8 * features * features),
            name="product",
        )(where, *lefts, *rights)
        parts = [parts[0]] + [swapped(parts[k], "band", k) for k in range(1, bands)]
        d_wkv_t = pl.pallas_call(
            total_kernel,
            out_shape=jax.ShapeDtypeStruct((block, features), F32),
            in_specs=[spec()] * bands,
            out_specs=spec(),
            name="total",
        )(*parts)
    else:
        product = lax.dot_general(
            partial_value, normed_window, (((0,), (0,)), ((), ())), preferred_element_type=F32
        )
        d_wkv_t = lax.psum_scatter(
            product * factor, ("band", "ens"), scatter_dimension=0, tiled=True
        )

    d_grid = pl.pallas_call(
        finish_kernel,
        out_shape=jax.ShapeDtypeStruct((rows, features), BF16),
        in_specs=[spec()] * 5,
        out_specs=spec(),
        scratch_shapes=[pltpu.VMEM((rows, features), F32)],
        cost_estimate=estimate(20 * rows * features, 8 * rows * features),
        name="finish",
    )(grid_latent, src_gain, d_own, back_low, back_high)
    return (updated[None], d_grid[None], d_wkv_t)


def solution(mesh):
    return jax.shard_map(
        per_device,
        mesh=mesh,
        in_specs=(
            P("ens", "band", None),
            P("ens", "band", None),
            P("ens", "band", None),
            P(),
            P(),
            P(),
            P(),
            P("band", None),
            P("band", None),
        ),
        out_specs=(P("ens", "band", None), P("ens", "band", None), P(("band", "ens"), None)),
        check_vma=False,
    )
```

```python
import functools
import math

import jax
import jax.numpy as jnp
from jax import lax
from jax.experimental import pallas as pl
from jax.experimental.pallas import tpu as pltpu
from jax.sharding import PartitionSpec as P

HEADS = 16
K = 12
R = 32
EPSILON = 1e-05
F32 = jnp.float32
BF16 = jnp.bfloat16


def spec(space=pltpu.VMEM):
    return pl.BlockSpec(memory_space=space)


def estimate(flops, moved):
    return pl.CostEstimate(flops=int(flops), bytes_accessed=int(moved), transcendentals=0)


def dot(left, right):
    return jnp.dot(left, right, preferred_element_type=F32)


def dot_rows(left, right):
    return lax.dot_general(left, right, (((0,), (0,)), ((), ())), preferred_element_type=F32)


def dot_lanes(left, right):
    return lax.dot_general(left, right, (((1,), (1,)), ((), ())), preferred_element_type=F32)


def halves(wide):
    high = wide.astype(BF16)
    return high, (wide - high.astype(F32)).astype(BF16)


def normalize(values):
    values = values.astype(F32)
    average = jnp.mean(values, axis=-1, keepdims=True)
    centred = values - average
    variance = jnp.mean(centred * centred, axis=-1, keepdims=True)
    inv_std = lax.rsqrt(variance + EPSILON)
    return centred * inv_std, inv_std


def parity():
    return lax.rem(lax.axis_index("band"), 2)


def pick(flag, one, zero):
    return flag * one + (1 - flag) * zero


def norm_kernel(grid_ref, gain_ref, normed_ref, edge_ref):
    standard, _ = normalize(grid_ref[...])
    normed_ref[...] = (standard * gain_ref[...]).astype(BF16)
    start = pl.multiple_of(pick(parity(), normed_ref.shape[0] - R, 0), R)
    edge_ref[...] = normed_ref[pl.ds(start, R)]


def query_kernel(hidden_ref, gain_ref, wq_ref, q_ref, hat_ref):
    @pl.when(pl.program_id(0) == 0)
    def _():
        standard, _ = normalize(hidden_ref[...])
        hat_ref[...] = (standard * gain_ref[...]).astype(BF16)

    q_ref[...] = dot(hat_ref[...], wq_ref[...]).astype(BF16)


def own_kernel(normed_ref, wkv_ref, kv_ref):
    kv_ref[...] = dot(normed_ref[...], wkv_ref[...]).astype(BF16)


def halo_kernel(outer_ref, pair_ref, far_ref, wkv_ref, kv_ref, shared_ref, both_ref):
    rows = pair_ref.shape[0]

    @pl.when(pl.program_id(0) == 0)
    def _():
        odd = parity()
        outer_at = pl.multiple_of(pick(odd, R, 0), R)
        inner_at = pl.multiple_of(pick(odd, 0, R), R)
        from_at = pl.multiple_of(pick(odd, rows - R, 0), R)
        both_ref[pl.ds(outer_at, R)] = outer_ref[...]
        both_ref[pl.ds(inner_at, R)] = pair_ref[pl.ds(from_at, R)]
        shared_ref[:rows] = pair_ref[...]
        shared_ref[rows : rows + R] = outer_ref[...]
        shared_ref[rows + R :] = far_ref[...]

    kv_ref[...] = dot(both_ref[...], wkv_ref[...]).astype(BF16)


def attend_kernel(
    halo_ref, kv_ref, q_ref, cot_ref, hidden_ref, index_ref, mask_ref, updated_ref, partial_ref,
    *refs
):
    piece_refs, window_ref = refs[:-1], refs[-1]
    nodes, features = q_ref.shape
    own = kv_ref.shape[0]
    rows = own + 2 * R
    lanes = 128
    head_dim = features // HEADS
    shift = head_dim.bit_length() - 1
    scale = 1.0 / math.sqrt(head_dim)
    window_ref[:R] = halo_ref[:R]
    window_ref[R : R + own] = kv_ref[...]
    window_ref[R + own :] = halo_ref[R:]

    eye_a = lax.broadcasted_iota(jnp.int32, (K, lanes), 0)
    eye_b = lax.broadcasted_iota(jnp.int32, (K, lanes), 1)
    eye = jnp.where(eye_a == eye_b, 1.0, 0.0).astype(BF16)
    first_row = lax.axis_index("band") * own - R
    local = dot_rows((index_ref[...] - first_row).astype(F32).astype(BF16), eye).astype(jnp.int32)
    mask = dot_rows(mask_ref[...].astype(F32).astype(BF16), eye)
    row_id = lax.broadcasted_iota(jnp.int32, (nodes, rows), 1)
    picks = jnp.concatenate(
        [jnp.where(row_id == local[:, k : k + 1], 1.0, 0.0).astype(BF16) for k in range(K)], axis=0
    )
    valid = jnp.concatenate([mask[:, k : k + 1] for k in range(K)], axis=0) > 0.5
    chunk = 256
    feature_id = lax.broadcasted_iota(jnp.int32, (features, lanes), 0)
    lane_id = lax.broadcasted_iota(jnp.int32, (features, lanes), 1)
    to_heads = jnp.where(jnp.right_shift(feature_id, shift) == lane_id, 1.0, 0.0).astype(BF16)
    lane_t = lax.broadcasted_iota(jnp.int32, (lanes, features), 0)
    feature_t = lax.broadcasted_iota(jnp.int32, (lanes, features), 1)
    from_heads = jnp.where(jnp.right_shift(feature_t, shift) == lane_t, 1.0, 0.0).astype(BF16)

    def repeated(ref, c):
        return jnp.broadcast_to(ref[:, c : c + chunk].astype(F32)[None], (K, nodes, chunk))

    def by_edge(ref, c, start):
        edge = dot(picks, window_ref[:, start + c : start + c + chunk])
        product = edge.reshape(K, nodes, chunk) * repeated(ref, c)
        first, second = halves(product.reshape(K * nodes, chunk))
        heads = to_heads[c : c + chunk]
        return dot(first, heads) + dot(second, heads)

    scores = by_edge(q_ref, 0, 0)
    d_probs = by_edge(cot_ref, 0, features)
    for c in range(chunk, features, chunk):
        scores = scores + by_edge(q_ref, c, 0)
        d_probs = d_probs + by_edge(cot_ref, c, features)
    scores = jnp.where(valid, scores * scale, -jnp.inf).reshape(K, nodes, lanes)
    d_probs = d_probs.reshape(K, nodes, lanes)
    terms = jnp.exp(scores - jnp.max(scores, axis=0, keepdims=True))
    probs = terms / jnp.sum(terms, axis=0, keepdims=True)
    probs_low = probs.reshape(K * nodes, lanes).astype(BF16)
    inner = jnp.sum(probs * d_probs, axis=0, keepdims=True)
    d_scores = (probs * (d_probs - inner)).reshape(K * nodes, lanes)
    d_first, d_second = halves(d_scores)

    for c in range(0, features, chunk):
        heads = from_heads[:, c : c + chunk]
        spread = dot(probs_low, heads).reshape(K, nodes, chunk)
        values = dot(picks, window_ref[:, features + c : features + c + chunk])
        attended = jnp.sum(spread * values.reshape(K, nodes, chunk), axis=0)
        updated_ref[:, c : c + chunk] = (
            hidden_ref[:, c : c + chunk].astype(F32) + attended
        ).astype(BF16)
        first, second = halves((spread * repeated(cot_ref, c)).reshape(K * nodes, chunk))
        partial_ref[:, features + c : features + c + chunk] = (
            dot_rows(picks, first) + dot_rows(picks, second)
        ).astype(BF16)
        spread = (dot(d_first, heads) + dot(d_second, heads)).reshape(K, nodes, chunk)
        keys = (spread * repeated(q_ref, c)).reshape(K * nodes, chunk) * scale
        first, second = halves(keys)
        partial_ref[:, c : c + chunk] = (
            dot_rows(picks, first) + dot_rows(picks, second)
        ).astype(BF16)

    mine = 2 * parity() + lax.axis_index("ens") // 2
    for k, piece_ref in enumerate(piece_refs):
        for i in range(piece_ref.shape[1] // lanes):
            start = pl.multiple_of((4 * i + (mine ^ k)) * lanes, lanes)
            piece_ref[:, i * lanes : (i + 1) * lanes] = partial_ref[:, pl.ds(start, lanes)]


def window_kernel(partial_ref, wkv_ref, own_ref, inner_ref, outer_ref, wide_ref):
    wide_ref[...] = dot_lanes(partial_ref[...], wkv_ref[...])
    rows = wide_ref.shape[0]
    odd = parity()
    inner_at = pl.multiple_of(pick(odd, 0, rows - R), R)
    outer_at = pl.multiple_of(pick(odd, rows - R, 0), R)
    own_ref[...] = wide_ref[R : rows - R]
    inner_ref[...] = wide_ref[pl.ds(inner_at, R)].astype(BF16)
    outer_ref[...] = wide_ref[pl.ds(outer_at, R)].astype(BF16)


def product_kernel(factor, *refs):
    lefts, (own, outer, pair, far, side, side_pair) = refs[:4], refs[4:10]
    keep_ref, send_ref, left_ref, right_ref, total_ref = refs[10:]
    window = lefts[0].shape[0]
    rows = own.shape[0]
    odd = parity()
    pieces = (
        ((own, 0), (outer, 0), (pair, 0)),
        ((side, 0), (side_pair, rows), (side_pair, 0)),
        ((pair, 0), (far, 0), (own, 0)),
        ((side_pair, 0), (side_pair, rows + R), (side, 0)),
    )
    for k, ((middle, m_at), (edge, e_at), (other, o_at)) in enumerate(pieces):
        base = k * window
        left_ref[base : base + window] = lefts[k][...]
        right_ref[base + R : base + R + rows] = middle[m_at : m_at + rows]
        flag = odd if k < 2 else 1 - odd
        edge_at = pl.multiple_of(base + pick(flag, R + rows, 0), R)
        other_at = pl.multiple_of(base + pick(flag, 0, R + rows), R)
        from_at = pl.multiple_of(o_at + pick(flag, rows - R, 0), R)
        right_ref[pl.ds(edge_at, R)] = edge[e_at : e_at + R]
        right_ref[pl.ds(other_at, R)] = other[pl.ds(from_at, R)]
    total_ref[...] = dot_rows(left_ref[...], right_ref[...]) * factor
    core = lax.rem(lax.axis_index("ens"), 2)
    block = keep_ref.shape[1]
    for i in range(keep_ref.shape[0]):
        keep_at = pl.multiple_of((2 * i + core) * block, block)
        send_at = pl.multiple_of((2 * i + 1 - core) * block, block)
        keep_ref[i] = total_ref[pl.ds(keep_at, block)]
        send_ref[i] = total_ref[pl.ds(send_at, block)].astype(BF16)


def pair_kernel(keep_ref, got_ref, *out_refs):
    group = lax.axis_index("band") // 2
    for k, out_ref in enumerate(out_refs):
        at = group ^ k
        out_ref[...] = (keep_ref[at] + got_ref[at].astype(F32)).astype(out_ref.dtype)


def finish_kernel(grid_ref, gain_ref, own_ref, inner_ref, outer_ref, out_ref, wide_ref):
    rows = own_ref.shape[0]
    odd = parity()
    wide_ref[...] = own_ref[...]
    inner_at = pl.multiple_of(pick(odd, 0, rows - R), R)
    outer_at = pl.multiple_of(pick(odd, rows - R, 0), R)
    wide_ref[pl.ds(inner_at, R)] = wide_ref[pl.ds(inner_at, R)] + inner_ref[...].astype(F32)
    wide_ref[pl.ds(outer_at, R)] = wide_ref[pl.ds(outer_at, R)] + outer_ref[...].astype(F32)
    standard, inv_std = normalize(grid_ref[...])
    scaled = wide_ref[...] * gain_ref[...]
    out_ref[...] = (
        inv_std
        * (
            scaled
            - jnp.mean(scaled, axis=-1, keepdims=True)
            - standard * jnp.mean(scaled * standard, axis=-1, keepdims=True)
        )
    ).astype(BF16)


def total_kernel(*refs):
    total = refs[0][...]
    for ref in refs[1:-1]:
        total = total + ref[...].astype(F32)
    refs[-1][...] = total


def swapped(value, band_bits, ens_bits):
    bands, members = lax.axis_size("band"), lax.axis_size("ens")
    flip = band_bits * members + ens_bits
    pairs = [(i, i ^ flip) for i in range(bands * members)]
    return lax.ppermute(value, ("band", "ens"), pairs)


def outward(value):
    bands = lax.axis_size("band")
    pairs = [(i, i + 1) for i in range(1, bands - 1, 2)]
    return lax.ppermute(value, "band", pairs + [(j, i) for i, j in pairs])


def call(kernel, name, shapes, operands, scratch=(), flops=0, moved=0, **options):
    if "in_specs" not in options:
        options["in_specs"] = [spec()] * len(operands)
        options["out_specs"] = [spec()] * len(shapes)
    return pl.pallas_call(
        kernel,
        out_shape=[jax.ShapeDtypeStruct(*shape) for shape in shapes],
        scratch_shapes=[pltpu.VMEM(*shape) for shape in scratch],
        cost_estimate=estimate(flops, moved),
        name=name,
        **options,
    )(*operands)


def streamed(kernel, name, steps, fixed, weight, shapes, scratch, flops):
    features, columns = weight.shape
    wide = columns // steps
    whole = [pl.BlockSpec(value.shape, lambda i: (0, 0)) for value in fixed]
    out = [pl.BlockSpec((shapes[0][0][0], wide), lambda i: (0, i))]
    out += [pl.BlockSpec(shape[0], lambda i: (0, 0)) for shape in shapes[1:]]
    return call(
        kernel, name, shapes, [*fixed, weight], scratch, flops, 2 * features * columns,
        grid=(steps,), in_specs=whole + [pl.BlockSpec((features, wide), lambda i: (0, i))],
        out_specs=out,
    )


def per_device(grid_latent, hidden, d_updated, w_kv, w_q, src_gain, q_gain, src_index, edge_mask):
    grid_latent, hidden, d_updated = grid_latent[0], hidden[0], d_updated[0]
    rows, features = grid_latent.shape
    nodes = hidden.shape[0]
    bands, members = lax.axis_size("band"), lax.axis_size("ens")
    window = rows + 2 * R
    block = 2 * features // (bands * members)
    groups = bands // 2
    src_gain, q_gain = src_gain[None], q_gain[None]
    grouped = members == 4 and groups & (groups - 1) == 0 and block == 64
    square = features * features

    normed, edge = call(
        norm_kernel, "norm", [((rows, features), BF16), ((R, features), BF16)],
        [grid_latent, src_gain], flops=10 * rows * features, moved=4 * rows * features,
    )
    outer = outward(edge)
    pair = swapped(normed, 1, 0)
    if grouped:
        side = swapped(normed, 0, 2)
    far = swapped(outer, 1, 0)

    (queries,) = streamed(
        query_kernel, "query", 2, [hidden, q_gain], w_q, [((nodes, features), BF16)],
        [((nodes, features), BF16)], 2 * nodes * square,
    )
    (kv,) = streamed(
        own_kernel, "own", 4, [normed], w_kv, [((rows, 2 * features), BF16)], [],
        4 * rows * square,
    )
    kv_halo, shared = streamed(
        halo_kernel, "halo", 4, [outer, pair, far], w_kv,
        [((2 * R, 2 * features), BF16), ((window, features), BF16)],
        [((2 * R, features), BF16)], 8 * R * square,
    )
    if grouped:
        side_pair = swapped(shared, 0, 2)

    pieces = 4 if grouped else 0
    updated, partial_value, *lefts = call(
        attend_kernel, "attend",
        [((nodes, features), BF16), ((window, 2 * features), BF16)]
        + [((window, features // 2), BF16)] * pieces,
        [kv_halo, kv, queries, d_updated, hidden, src_index.T, edge_mask.T],
        [((window, 2 * features), BF16)], flops=3e9, moved=4 * square,
    )
    if grouped:
        lefts = [lefts[0], swapped(lefts[1], 0, 2), swapped(lefts[2], 1, 0), swapped(lefts[3], 1, 2)]

    d_own, d_inner, d_outer = call(
        window_kernel, "window",
        [((rows, features), F32), ((R, features), BF16), ((R, features), BF16)],
        [partial_value, w_kv], [((window, features), F32)],
        flops=4 * window * square, moved=4 * square,
    )
    d_inner = swapped(d_inner, 1, 0)
    d_outer = outward(d_outer)

    factor = 1.0 / math.sqrt(members * rows * bands)
    if grouped:
        keep, send = call(
            functools.partial(product_kernel, factor), "product",
            [((groups, block, features), F32), ((groups, block, features), BF16)],
            [*lefts, normed, outer, pair, far, side, side_pair],
            [
                ((4 * window, features // 2), BF16),
                ((4 * window, features), BF16),
                ((features // 2, features), F32),
            ],
            flops=4 * window * square, moved=4 * square,
        )
        got = swapped(send, 0, 1)
        parts = call(
            pair_kernel, "pair",
            [((block, features), F32)] + [((block, features), BF16)] * (groups - 1),
            [keep, got], flops=square, moved=4 * square,
        )
        parts = [parts[0]] + [swapped(parts[k], 2 * k, 0) for k in range(1, groups)]
        (d_wkv_t,) = call(total_kernel, "total", [((block, features), F32)], parts)
    else:
        odd = lax.rem(lax.axis_index("band"), 2) == 1
        low = jnp.where(odd, pair[rows - R :], outer)
        high = jnp.where(odd, outer, pair[:R])
        normed_window = jnp.concatenate([low, normed, high], axis=0)
        d_wkv_t = lax.psum_scatter(
            dot_rows(partial_value, normed_window) * factor,
            ("band", "ens"), scatter_dimension=0, tiled=True,
        )

    (d_grid,) = call(
        finish_kernel, "finish", [((rows, features), BF16)],
        [grid_latent, src_gain, d_own, d_inner, d_outer], [((rows, features), F32)],
        flops=20 * rows * features, moved=8 * rows * features,
    )
    return (updated[None], d_grid[None], d_wkv_t)


def solution(mesh):
    return jax.shard_map(
        per_device,
        mesh=mesh,
        in_specs=(
            P("ens", "band", None),
            P("ens", "band", None),
            P("ens", "band", None),
            P(),
            P(),
            P(),
            P(),
            P("band", None),
            P("band", None),
        ),
        out_specs=(P("ens", "band", None), P("ens", "band", None), P(("band", "ens"), None)),
        check_vma=False,
    )
```

```python
import functools
import math

import jax
import jax.numpy as jnp
from jax import lax
from jax.experimental import pallas as pl
from jax.experimental.pallas import tpu as pltpu
from jax.sharding import PartitionSpec as P

HEADS = 16
K = 12
R = 32
EPSILON = 1e-05
LIMIT = 24 << 20
F32 = jnp.float32
BF16 = jnp.bfloat16


def spec(space=pltpu.VMEM):
    return pl.BlockSpec(memory_space=space)


def estimate(flops, moved):
    return pl.CostEstimate(flops=int(flops), bytes_accessed=int(moved), transcendentals=0)


def dot(left, right):
    return jnp.dot(left, right, preferred_element_type=F32)


def dot_rows(left, right):
    return lax.dot_general(left, right, (((0,), (0,)), ((), ())), preferred_element_type=F32)


def dot_lanes(left, right):
    return lax.dot_general(left, right, (((1,), (1,)), ((), ())), preferred_element_type=F32)


def halves(wide):
    high = wide.astype(BF16)
    return high, (wide - high.astype(F32)).astype(BF16)


def normalize(values):
    values = values.astype(F32)
    average = jnp.mean(values, axis=-1, keepdims=True)
    centred = values - average
    variance = jnp.mean(centred * centred, axis=-1, keepdims=True)
    inv_std = lax.rsqrt(variance + EPSILON)
    return centred * inv_std, inv_std


def parity():
    return lax.rem(lax.axis_index("band"), 2)


def pick(flag, one, zero):
    return flag * one + (1 - flag) * zero


def norm_kernel(grid_ref, gain_ref, normed_ref, edge_ref):
    standard, _ = normalize(grid_ref[...])
    normed_ref[...] = (standard * gain_ref[...]).astype(BF16)
    start = pl.multiple_of(pick(parity(), normed_ref.shape[0] - R, 0), R)
    edge_ref[...] = normed_ref[pl.ds(start, R)]


def project_kernel(hidden_ref, gain_ref, wq_ref, normed_ref, wkv_ref, q_ref, kv_ref):
    standard, _ = normalize(hidden_ref[...])
    hat = (standard * gain_ref[...]).astype(BF16)
    q_ref[...] = dot(hat, wq_ref[...]).astype(BF16)
    kv_ref[...] = dot(normed_ref[...], wkv_ref[...]).astype(BF16)


def attend_kernel(
    outer_ref, pair_ref, wkv_ref, kv_ref, q_ref, cot_ref, hidden_ref, index_ref, mask_ref,
    updated_ref, partial_ref, *refs
):
    piece_refs, (both_ref, halo_ref, window_ref) = refs[:-3], refs[-3:]
    nodes, features = q_ref.shape
    own = kv_ref.shape[0]
    rows = own + 2 * R
    lanes = 128
    head_dim = features // HEADS
    shift = head_dim.bit_length() - 1
    scale = 1.0 / math.sqrt(head_dim)
    odd = parity()
    outer_at = pl.multiple_of(pick(odd, R, 0), R)
    inner_at = pl.multiple_of(pick(odd, 0, R), R)
    from_at = pl.multiple_of(pick(odd, own - R, 0), R)
    both_ref[pl.ds(outer_at, R)] = outer_ref[...]
    both_ref[pl.ds(inner_at, R)] = pair_ref[pl.ds(from_at, R)]
    halo_ref[...] = dot(both_ref[...], wkv_ref[...]).astype(BF16)
    window_ref[:R] = halo_ref[:R]
    window_ref[R : R + own] = kv_ref[...]
    window_ref[R + own :] = halo_ref[R:]

    eye_a = lax.broadcasted_iota(jnp.int32, (K, lanes), 0)
    eye_b = lax.broadcasted_iota(jnp.int32, (K, lanes), 1)
    eye = jnp.where(eye_a == eye_b, 1.0, 0.0).astype(BF16)
    first_row = lax.axis_index("band") * own - R
    local = dot_rows((index_ref[...] - first_row).astype(F32).astype(BF16), eye).astype(jnp.int32)
    mask = dot_rows(mask_ref[...].astype(F32).astype(BF16), eye)
    row_id = lax.broadcasted_iota(jnp.int32, (nodes, rows), 1)
    picks = jnp.concatenate(
        [jnp.where(row_id == local[:, k : k + 1], 1.0, 0.0).astype(BF16) for k in range(K)], axis=0
    )
    valid = jnp.concatenate([mask[:, k : k + 1] for k in range(K)], axis=0) > 0.5
    chunk = 256
    feature_id = lax.broadcasted_iota(jnp.int32, (features, lanes), 0)
    lane_id = lax.broadcasted_iota(jnp.int32, (features, lanes), 1)
    to_heads = jnp.where(jnp.right_shift(feature_id, shift) == lane_id, 1.0, 0.0).astype(BF16)
    lane_t = lax.broadcasted_iota(jnp.int32, (lanes, features), 0)
    feature_t = lax.broadcasted_iota(jnp.int32, (lanes, features), 1)
    from_heads = jnp.where(jnp.right_shift(feature_t, shift) == lane_t, 1.0, 0.0).astype(BF16)

    def repeated(ref, c):
        return jnp.broadcast_to(ref[:, c : c + chunk].astype(F32)[None], (K, nodes, chunk))

    def by_edge(ref, c, start):
        edge = dot(picks, window_ref[:, start + c : start + c + chunk])
        product = edge.reshape(K, nodes, chunk) * repeated(ref, c)
        first, second = halves(product.reshape(K * nodes, chunk))
        heads = to_heads[c : c + chunk]
        return dot(first, heads) + dot(second, heads)

    scores = by_edge(q_ref, 0, 0)
    d_probs = by_edge(cot_ref, 0, features)
    for c in range(chunk, features, chunk):
        scores = scores + by_edge(q_ref, c, 0)
        d_probs = d_probs + by_edge(cot_ref, c, features)
    scores = jnp.where(valid, scores * scale, -jnp.inf).reshape(K, nodes, lanes)
    d_probs = d_probs.reshape(K, nodes, lanes)
    terms = jnp.exp(scores - jnp.max(scores, axis=0, keepdims=True))
    probs = terms / jnp.sum(terms, axis=0, keepdims=True)
    probs_low = probs.reshape(K * nodes, lanes).astype(BF16)
    inner = jnp.sum(probs * d_probs, axis=0, keepdims=True)
    d_scores = (probs * (d_probs - inner)).reshape(K * nodes, lanes)
    d_first, d_second = halves(d_scores)

    for c in range(0, features, chunk):
        heads = from_heads[:, c : c + chunk]
        spread = dot(probs_low, heads).reshape(K, nodes, chunk)
        values = dot(picks, window_ref[:, features + c : features + c + chunk])
        attended = jnp.sum(spread * values.reshape(K, nodes, chunk), axis=0)
        updated_ref[:, c : c + chunk] = (
            hidden_ref[:, c : c + chunk].astype(F32) + attended
        ).astype(BF16)
        first, second = halves((spread * repeated(cot_ref, c)).reshape(K * nodes, chunk))
        partial_ref[:, features + c : features + c + chunk] = (
            dot_rows(picks, first) + dot_rows(picks, second)
        ).astype(BF16)
        spread = (dot(d_first, heads) + dot(d_second, heads)).reshape(K, nodes, chunk)
        keys = (spread * repeated(q_ref, c)).reshape(K * nodes, chunk) * scale
        first, second = halves(keys)
        partial_ref[:, c : c + chunk] = (
            dot_rows(picks, first) + dot_rows(picks, second)
        ).astype(BF16)

    mine = 2 * odd + lax.axis_index("ens") // 2
    core = lax.rem(lax.axis_index("ens"), 2)
    half = lanes // 2
    left = lax.broadcasted_iota(jnp.int32, (rows, lanes), 1) < half
    for k, piece_ref in enumerate(piece_refs):
        count = piece_ref.shape[1] // lanes
        for i in range(count // 2):
            tiles = []
            for t in (2 * i, 2 * i + 1):
                start = pl.multiple_of((4 * t + (mine ^ k)) * lanes, lanes)
                tiles.append(partial_ref[:, pl.ds(start, lanes)].astype(F32))
            one, two = tiles
            firsts = jnp.where(left, one, pltpu.roll(two, half, 1)).astype(BF16)
            seconds = jnp.where(left, pltpu.roll(one, half, 1), two).astype(BF16)
            first_at = pl.multiple_of((pick(core, 0, count // 2) + i) * lanes, lanes)
            second_at = pl.multiple_of((pick(core, count // 2, 0) + i) * lanes, lanes)
            piece_ref[:, pl.ds(first_at, lanes)] = firsts
            piece_ref[:, pl.ds(second_at, lanes)] = seconds


def window_kernel(partial_ref, wkv_ref, own_ref, inner_ref, outer_ref, wide_ref):
    wide_ref[...] = dot_lanes(partial_ref[...], wkv_ref[...])
    rows = wide_ref.shape[0]
    odd = parity()
    inner_at = pl.multiple_of(pick(odd, 0, rows - R), R)
    outer_at = pl.multiple_of(pick(odd, rows - R, 0), R)
    own_ref[...] = wide_ref[R : rows - R]
    inner_ref[...] = wide_ref[pl.ds(inner_at, R)].astype(BF16)
    outer_ref[...] = wide_ref[pl.ds(outer_at, R)].astype(BF16)


def product_kernel(factor, start, *refs):
    lefts, (own, outer, pair, far, side, side_pair) = refs[:4], refs[4:10]
    out_ref, left_ref, right_ref = refs[10:]
    columns = left_ref.shape[1]
    window = lefts[0].shape[0]
    rows = own.shape[0]
    odd = parity()
    pieces = (
        ((own, 0), (outer, 0), (pair, 0)),
        ((side, 0), (side_pair, rows), (side_pair, 0)),
        ((pair, 0), (far, 0), (own, 0)),
        ((side_pair, 0), (side_pair, rows + R), (side, 0)),
    )
    for k, ((middle, m_at), (edge, e_at), (other, o_at)) in enumerate(pieces):
        base = k * window
        left_ref[base : base + window] = lefts[k][:, start : start + columns]
        right_ref[base + R : base + R + rows] = middle[m_at : m_at + rows]
        flag = odd if k < 2 else 1 - odd
        edge_at = pl.multiple_of(base + pick(flag, R + rows, 0), R)
        other_at = pl.multiple_of(base + pick(flag, 0, R + rows), R)
        from_at = pl.multiple_of(o_at + pick(flag, rows - R, 0), R)
        right_ref[pl.ds(edge_at, R)] = edge[e_at : e_at + R]
        right_ref[pl.ds(other_at, R)] = other[pl.ds(from_at, R)]
    total = dot_rows(left_ref[...], right_ref[...]) * factor
    out_ref[...] = total.astype(out_ref.dtype)


def pair_kernel(keep_ref, got_ref, *out_refs):
    group = lax.axis_index("band") // 2
    block = out_refs[0].shape[0]
    for k, out_ref in enumerate(out_refs):
        at = pl.ds(pl.multiple_of((group ^ k) * block, block), block)
        out_ref[...] = (keep_ref[at] + got_ref[at].astype(F32)).astype(out_ref.dtype)


def finish_kernel(grid_ref, gain_ref, own_ref, inner_ref, outer_ref, out_ref, wide_ref):
    rows = own_ref.shape[0]
    odd = parity()
    wide_ref[...] = own_ref[...]
    inner_at = pl.multiple_of(pick(odd, 0, rows - R), R)
    outer_at = pl.multiple_of(pick(odd, rows - R, 0), R)
    wide_ref[pl.ds(inner_at, R)] = wide_ref[pl.ds(inner_at, R)] + inner_ref[...].astype(F32)
    wide_ref[pl.ds(outer_at, R)] = wide_ref[pl.ds(outer_at, R)] + outer_ref[...].astype(F32)
    standard, inv_std = normalize(grid_ref[...])
    scaled = wide_ref[...] * gain_ref[...]
    out_ref[...] = (
        inv_std
        * (
            scaled
            - jnp.mean(scaled, axis=-1, keepdims=True)
            - standard * jnp.mean(scaled * standard, axis=-1, keepdims=True)
        )
    ).astype(BF16)


def total_kernel(*refs):
    total = refs[0][...]
    for ref in refs[1:-1]:
        total = total + ref[...].astype(F32)
    refs[-1][...] = total


def swapped(value, band_bits, ens_bits):
    bands, members = lax.axis_size("band"), lax.axis_size("ens")
    flip = band_bits * members + ens_bits
    pairs = [(i, i ^ flip) for i in range(bands * members)]
    return lax.ppermute(value, ("band", "ens"), pairs)


def outward(value):
    bands = lax.axis_size("band")
    pairs = [(i, i + 1) for i in range(1, bands - 1, 2)]
    return lax.ppermute(value, "band", pairs + [(j, i) for i, j in pairs])


def beyond(value):
    bands = lax.axis_size("band")
    pairs = [(i, i + 2) for i in range(1, bands - 2, 2)]
    return lax.ppermute(value, "band", pairs + [(i + 2, i) for i in range(0, bands - 2, 2)])


def call(kernel, name, shapes, operands, scratch=(), flops=0, moved=0, **options):
    if "in_specs" not in options:
        options["in_specs"] = [spec()] * len(operands)
        options["out_specs"] = [spec()] * len(shapes)
    return pl.pallas_call(
        kernel,
        out_shape=[jax.ShapeDtypeStruct(*shape) for shape in shapes],
        scratch_shapes=[pltpu.VMEM(*shape) for shape in scratch],
        cost_estimate=estimate(flops, moved),
        compiler_params=pltpu.CompilerParams(vmem_limit_bytes=LIMIT),
        name=name,
        **options,
    )(*operands)


def per_device(grid_latent, hidden, d_updated, w_kv, w_q, src_gain, q_gain, src_index, edge_mask):
    grid_latent, hidden, d_updated = grid_latent[0], hidden[0], d_updated[0]
    rows, features = grid_latent.shape
    nodes = hidden.shape[0]
    bands, members = lax.axis_size("band"), lax.axis_size("ens")
    window = rows + 2 * R
    block = 2 * features // (bands * members)
    groups = bands // 2
    src_gain, q_gain = src_gain[None], q_gain[None]
    grouped = members == 4 and groups & (groups - 1) == 0 and block == 64
    square = features * features

    normed, edge = call(
        norm_kernel, "norm", [((rows, features), BF16), ((R, features), BF16)],
        [grid_latent, src_gain], flops=10 * rows * features, moved=4 * rows * features,
    )
    outer = outward(edge)
    pair = swapped(normed, 1, 0)
    if grouped:
        side = swapped(normed, 0, 2)
    far = beyond(edge)

    queries, kv = call(
        project_kernel, "project", [((nodes, features), BF16), ((rows, 2 * features), BF16)],
        [hidden, q_gain, w_q, normed, w_kv], flops=2 * (2 * rows + nodes) * square, moved=6 * square,
    )
    if grouped:
        side_pair = swapped(jnp.concatenate([pair, outer, far], axis=0), 0, 2)

    pieces = 4 if grouped else 0
    updated, partial_value, *lefts = call(
        attend_kernel, "attend",
        [((nodes, features), BF16), ((window, 2 * features), BF16)]
        + [((window, features // 2), BF16)] * pieces,
        [outer, pair, w_kv, kv, queries, d_updated, hidden, src_index.T, edge_mask.T],
        [
            ((2 * R, features), BF16), ((2 * R, 2 * features), BF16),
            ((window, 2 * features), BF16),
        ],
        flops=3e9, moved=4 * square,
    )
    if grouped:
        lefts = [lefts[0], swapped(lefts[1], 0, 2), swapped(lefts[2], 1, 0), swapped(lefts[3], 1, 2)]

    d_own, d_inner, d_outer = call(
        window_kernel, "window",
        [((rows, features), F32), ((R, features), BF16), ((R, features), BF16)],
        [partial_value, w_kv], [((window, features), F32)],
        flops=4 * window * square, moved=4 * square,
    )
    d_inner = swapped(d_inner, 1, 0)
    d_outer = outward(d_outer)

    factor = 1.0 / math.sqrt(members * rows * bands)
    if grouped:
        operands = [*lefts, normed, outer, pair, far, side, side_pair]
        columns = features // 4
        buffers = [((4 * window, columns), BF16), ((4 * window, features), BF16)]
        (send,) = call(
            functools.partial(product_kernel, factor, 0), "product_send",
            [((columns, features), BF16)], operands, buffers,
            flops=2 * window * square, moved=4 * square,
        )
        got = swapped(send, 0, 1)
        (keep,) = call(
            functools.partial(product_kernel, factor, columns), "product_keep",
            [((columns, features), F32)], operands, buffers,
            flops=2 * window * square, moved=4 * square,
        )
        parts = call(
            pair_kernel, "pair",
            [((block, features), F32)] + [((block, features), BF16)] * (groups - 1),
            [keep, got], flops=square, moved=4 * square,
        )
        parts = [parts[0]] + [swapped(parts[k], 2 * k, 0) for k in range(1, groups)]
        (d_wkv_t,) = call(total_kernel, "total", [((block, features), F32)], parts)
    else:
        odd = lax.rem(lax.axis_index("band"), 2) == 1
        low = jnp.where(odd, pair[rows - R :], outer)
        high = jnp.where(odd, outer, pair[:R])
        normed_window = jnp.concatenate([low, normed, high], axis=0)
        d_wkv_t = lax.psum_scatter(
            dot_rows(partial_value, normed_window) * factor,
            ("band", "ens"), scatter_dimension=0, tiled=True,
        )

    (d_grid,) = call(
        finish_kernel, "finish", [((rows, features), BF16)],
        [grid_latent, src_gain, d_own, d_inner, d_outer], [((rows, features), F32)],
        flops=20 * rows * features, moved=8 * rows * features,
    )
    return (updated[None], d_grid[None], d_wkv_t)


def solution(mesh):
    return jax.shard_map(
        per_device,
        mesh=mesh,
        in_specs=(
            P("ens", "band", None),
            P("ens", "band", None),
            P("ens", "band", None),
            P(),
            P(),
            P(),
            P(),
            P("band", None),
            P("band", None),
        ),
        out_specs=(P("ens", "band", None), P("ens", "band", None), P(("band", "ens"), None)),
        check_vma=False,
    )
```

```python
import functools
import math

import jax
import jax.numpy as jnp
from jax import lax
from jax.experimental import pallas as pl
from jax.experimental.pallas import tpu as pltpu
from jax.sharding import PartitionSpec as P

HEADS = 16
K = 12
R = 32
EPSILON = 1e-05
SLOTS = 16
LIMIT = 24 << 20
F32 = jnp.float32
BF16 = jnp.bfloat16


def spec(space=pltpu.VMEM):
    return pl.BlockSpec(memory_space=space)


def estimate(flops, moved):
    return pl.CostEstimate(flops=int(flops), bytes_accessed=int(moved), transcendentals=0)


def dot(left, right):
    return jnp.dot(left, right, preferred_element_type=F32)


def dot_rows(left, right):
    return lax.dot_general(left, right, (((0,), (0,)), ((), ())), preferred_element_type=F32)


def dot_lanes(left, right):
    return lax.dot_general(left, right, (((1,), (1,)), ((), ())), preferred_element_type=F32)


def halves(wide):
    high = wide.astype(BF16)
    return high, (wide - high.astype(F32)).astype(BF16)


def normalize(values):
    values = values.astype(F32)
    average = jnp.mean(values, axis=-1, keepdims=True)
    centred = values - average
    variance = jnp.mean(centred * centred, axis=-1, keepdims=True)
    inv_std = lax.rsqrt(variance + EPSILON)
    return centred * inv_std, inv_std


def parity():
    return lax.rem(lax.axis_index("band"), 2)


def pick(flag, one, zero):
    return flag * one + (1 - flag) * zero


def norm_kernel(grid_ref, gain_ref, normed_ref, edge_ref):
    standard, _ = normalize(grid_ref[...])
    normed_ref[...] = (standard * gain_ref[...]).astype(BF16)
    start = pl.multiple_of(pick(parity(), normed_ref.shape[0] - R, 0), R)
    edge_ref[...] = normed_ref[pl.ds(start, R)]


def project_kernel(hidden_ref, gain_ref, wq_ref, normed_ref, wkv_ref, q_ref, kv_ref):
    standard, _ = normalize(hidden_ref[...])
    hat = (standard * gain_ref[...]).astype(BF16)
    q_ref[...] = dot(hat, wq_ref[...]).astype(BF16)
    kv_ref[...] = dot(normed_ref[...], wkv_ref[...]).astype(BF16)


def picked(local, rows):
    row_id = lax.broadcasted_iota(jnp.int32, (local.shape[0], rows), 1)
    return jnp.concatenate(
        [jnp.where(row_id == local[:, k : k + 1], 1.0, 0.0).astype(BF16) for k in range(K)], axis=0
    )


def attend_kernel(
    outer_ref, pair_ref, wkv_ref, kv_ref, q_ref, cot_ref, hidden_ref, index_ref, mask_ref,
    updated_ref, partial_ref, *refs
):
    piece_refs, (both_ref, halo_ref, window_ref) = refs[:-3], refs[-3:]
    piece_ref, packet_refs = piece_refs[:1], piece_refs[1:]
    nodes, features = q_ref.shape
    own = kv_ref.shape[0]
    rows = own + 2 * R
    lanes = 128
    head_dim = features // HEADS
    shift = head_dim.bit_length() - 1
    scale = 1.0 / math.sqrt(head_dim)
    odd = parity()
    outer_at = pl.multiple_of(pick(odd, R, 0), R)
    inner_at = pl.multiple_of(pick(odd, 0, R), R)
    from_at = pl.multiple_of(pick(odd, own - R, 0), R)
    both_ref[pl.ds(outer_at, R)] = outer_ref[...]
    both_ref[pl.ds(inner_at, R)] = pair_ref[pl.ds(from_at, R)]
    halo_ref[...] = dot(both_ref[...], wkv_ref[...]).astype(BF16)
    window_ref[:R] = halo_ref[:R]
    window_ref[R : R + own] = kv_ref[...]
    window_ref[R + own :] = halo_ref[R:]

    eye_a = lax.broadcasted_iota(jnp.int32, (K, lanes), 0)
    eye_b = lax.broadcasted_iota(jnp.int32, (K, lanes), 1)
    eye = jnp.where(eye_a == eye_b, 1.0, 0.0).astype(BF16)
    first_row = lax.axis_index("band") * own - R
    rows_low = (index_ref[...] - first_row).astype(F32).astype(BF16)
    local = dot_rows(rows_low, eye).astype(jnp.int32)
    mask = dot_rows(mask_ref[...].astype(F32).astype(BF16), eye)
    picks = picked(local, rows)
    valid = jnp.concatenate([mask[:, k : k + 1] for k in range(K)], axis=0) > 0.5
    chunk = 256
    feature_id = lax.broadcasted_iota(jnp.int32, (features, lanes), 0)
    lane_id = lax.broadcasted_iota(jnp.int32, (features, lanes), 1)
    to_heads = jnp.where(jnp.right_shift(feature_id, shift) == lane_id, 1.0, 0.0).astype(BF16)
    lane_t = lax.broadcasted_iota(jnp.int32, (lanes, features), 0)
    feature_t = lax.broadcasted_iota(jnp.int32, (lanes, features), 1)
    from_heads = jnp.where(jnp.right_shift(feature_t, shift) == lane_t, 1.0, 0.0).astype(BF16)

    def repeated(ref, c):
        return jnp.broadcast_to(ref[:, c : c + chunk].astype(F32)[None], (K, nodes, chunk))

    def by_edge(ref, c, start):
        edge = dot(picks, window_ref[:, start + c : start + c + chunk])
        product = edge.reshape(K, nodes, chunk) * repeated(ref, c)
        first, second = halves(product.reshape(K * nodes, chunk))
        heads = to_heads[c : c + chunk]
        return dot(first, heads) + dot(second, heads)

    scores = by_edge(q_ref, 0, 0)
    d_probs = by_edge(cot_ref, 0, features)
    for c in range(chunk, features, chunk):
        scores = scores + by_edge(q_ref, c, 0)
        d_probs = d_probs + by_edge(cot_ref, c, features)
    scores = jnp.where(valid, scores * scale, -jnp.inf).reshape(K, nodes, lanes)
    d_probs = d_probs.reshape(K, nodes, lanes)
    terms = jnp.exp(scores - jnp.max(scores, axis=0, keepdims=True))
    probs = terms / jnp.sum(terms, axis=0, keepdims=True)
    probs_low = probs.reshape(K * nodes, lanes).astype(BF16)
    inner = jnp.sum(probs * d_probs, axis=0, keepdims=True)
    d_scores = (probs * (d_probs - inner)).reshape(K * nodes, lanes) * scale
    d_first, d_second = halves(d_scores)

    for c in range(0, features, chunk):
        heads = from_heads[:, c : c + chunk]
        spread = dot(probs_low, heads).reshape(K, nodes, chunk)
        values = dot(picks, window_ref[:, features + c : features + c + chunk])
        attended = jnp.sum(spread * values.reshape(K, nodes, chunk), axis=0)
        updated_ref[:, c : c + chunk] = (
            hidden_ref[:, c : c + chunk].astype(F32) + attended
        ).astype(BF16)
        first, second = halves((spread * repeated(cot_ref, c)).reshape(K * nodes, chunk))
        partial_ref[:, features + c : features + c + chunk] = (
            dot_rows(picks, first) + dot_rows(picks, second)
        ).astype(BF16)
        spread = (dot(d_first, heads) + dot(d_second, heads)).reshape(K, nodes, chunk)
        first, second = halves((spread * repeated(q_ref, c)).reshape(K * nodes, chunk))
        partial_ref[:, c : c + chunk] = (
            dot_rows(picks, first) + dot_rows(picks, second)
        ).astype(BF16)

    mine = 2 * odd + lax.axis_index("ens") // 2
    core = lax.rem(lax.axis_index("ens"), 2)
    def arranged(sources, out_ref, row, group):
        count = sources[0].shape[0]
        left = lax.broadcasted_iota(jnp.int32, (count, lanes), 1) < head_dim
        for i in range(2):
            source = sources[i % len(sources)]
            shift_by = i * features if len(sources) == 1 else 0
            tiles = []
            for t in range(2):
                start = pl.multiple_of(shift_by + (4 * t + group) * lanes, lanes)
                tiles.append(source[:, pl.ds(start, lanes)].astype(F32))
            one, two = tiles
            firsts = jnp.where(left, one, pltpu.roll(two, head_dim, 1)).astype(BF16)
            seconds = jnp.where(left, pltpu.roll(one, head_dim, 1), two).astype(BF16)
            first_at = pl.multiple_of((pick(core, 0, 2) + i) * lanes, lanes)
            second_at = pl.multiple_of((pick(core, 2, 0) + i) * lanes, lanes)
            out_ref[row : row + count, pl.ds(first_at, lanes)] = firsts
            out_ref[row : row + count, pl.ds(second_at, lanes)] = seconds

    if piece_ref:
        arranged([partial_ref], piece_ref[0], 0, mine)
    row_r = lax.broadcasted_iota(jnp.int32, (SLOTS, lanes), 0)
    lane_r = lax.broadcasted_iota(jnp.int32, (SLOTS, lanes), 1)
    keep = jnp.bitwise_and(jnp.right_shift(row_r, 1), 1)
    head_r = jnp.where(keep == 1, core, 1 - core) + (HEADS // 2) * jnp.bitwise_and(row_r, 1)
    for k, packet_ref in enumerate(packet_refs):
        group = mine ^ (k + 1)
        chosen = lane_r == head_r + 2 * group
        factors = jnp.zeros((SLOTS, K * nodes), F32)
        for kind, values in enumerate((probs_low, d_first, d_second)):
            select = jnp.where(jnp.right_shift(row_r, 2) == kind, jnp.where(chosen, 1.0, 0.0), 0.0)
            factors = factors + dot_lanes(select.astype(BF16), values)
        packet_ref[:SLOTS, : K * nodes] = factors.astype(BF16)
        packet_ref[:SLOTS, K * nodes :] = jnp.zeros((SLOTS, 4 * lanes - K * nodes), BF16)
        packet_ref[:K, K * nodes : K * nodes + nodes] = rows_low
        arranged([q_ref, cot_ref], packet_ref, SLOTS, group)


def window_kernel(partial_ref, wkv_ref, own_ref, inner_ref, outer_ref, wide_ref):
    wide_ref[...] = dot_lanes(partial_ref[...], wkv_ref[...])
    rows = wide_ref.shape[0]
    odd = parity()
    inner_at = pl.multiple_of(pick(odd, 0, rows - R), R)
    outer_at = pl.multiple_of(pick(odd, rows - R, 0), R)
    own_ref[...] = wide_ref[R : rows - R]
    inner_ref[...] = wide_ref[pl.ds(inner_at, R)].astype(BF16)
    outer_ref[...] = wide_ref[pl.ds(outer_at, R)].astype(BF16)


def product_kernel(factor, start, *refs):
    lefts, (own, outer, pair, far, side, side_pair) = refs[:4], refs[4:10]
    out_ref, left_ref, right_ref = refs[10:]
    window, columns = lefts[0].shape[0], left_ref.shape[1]
    nodes = lefts[1].shape[0] - SLOTS
    edges, lanes, shift = K * nodes, 128, (columns // 4).bit_length() - 1
    row_r = lax.broadcasted_iota(jnp.int32, (SLOTS, columns), 0)
    part = jnp.right_shift(lax.broadcasted_iota(jnp.int32, (SLOTS, columns), 1), shift)
    kind = jnp.minimum(jnp.right_shift(row_r, 2), 1)
    wanted = 2 * (start // columns) + jnp.bitwise_and(part, 1)
    expand = jnp.where(jnp.bitwise_and(row_r, 3) == wanted, 1.0, 0.0)
    expand = jnp.where(kind == 1 - jnp.right_shift(part, 1), expand, 0.0)
    expand = jnp.where(row_r < 12, expand, 0.0).astype(BF16)
    eye_a = lax.broadcasted_iota(jnp.int32, (SLOTS, lanes), 0)
    eye_b = lax.broadcasted_iota(jnp.int32, (SLOTS, lanes), 1)
    eye = jnp.where(eye_a == eye_b, 1.0, 0.0).astype(BF16)
    left_ref[:window] = lefts[0][:, start : start + columns]
    for k in range(1, 4):
        packet = lefts[k]
        if k < 3:
            local = dot_rows(packet[:SLOTS, edges:], eye)[:nodes].astype(jnp.int32)
            picks = picked(local, window)
        spread = dot_rows(packet[:SLOTS, :edges], expand).reshape(K, nodes, columns)
        given = packet[SLOTS:, start : start + columns].astype(F32)
        first, second = halves((spread * given[None]).reshape(edges, columns))
        left_ref[k * window : (k + 1) * window] = (
            dot_rows(picks, first) + dot_rows(picks, second)
        ).astype(BF16)
    rows = own.shape[0]
    odd = parity()
    pieces = (
        ((own, 0), (outer, 0), (pair, 0)),
        ((side, 0), (side_pair, rows), (side_pair, 0)),
        ((pair, 0), (far, 0), (own, 0)),
        ((side_pair, 0), (side_pair, rows + R), (side, 0)),
    )
    for k, ((middle, m_at), (edge, e_at), (other, o_at)) in enumerate(pieces):
        base = k * window
        right_ref[base + R : base + R + rows] = middle[m_at : m_at + rows]
        flag = odd if k < 2 else 1 - odd
        edge_at = pl.multiple_of(base + pick(flag, R + rows, 0), R)
        other_at = pl.multiple_of(base + pick(flag, 0, R + rows), R)
        from_at = pl.multiple_of(o_at + pick(flag, rows - R, 0), R)
        right_ref[pl.ds(edge_at, R)] = edge[e_at : e_at + R]
        right_ref[pl.ds(other_at, R)] = other[pl.ds(from_at, R)]
    total = dot_rows(left_ref[...], right_ref[...]) * factor
    out_ref[...] = total.astype(out_ref.dtype)


def pair_kernel(keep_ref, got_ref, *out_refs):
    group = lax.axis_index("band") // 2
    block = out_refs[0].shape[0]
    for k, out_ref in enumerate(out_refs):
        at = pl.ds(pl.multiple_of((group ^ k) * block, block), block)
        out_ref[...] = (keep_ref[at] + got_ref[at].astype(F32)).astype(out_ref.dtype)


def finish_kernel(grid_ref, gain_ref, own_ref, inner_ref, outer_ref, out_ref, wide_ref):
    rows = own_ref.shape[0]
    odd = parity()
    wide_ref[...] = own_ref[...]
    inner_at = pl.multiple_of(pick(odd, 0, rows - R), R)
    outer_at = pl.multiple_of(pick(odd, rows - R, 0), R)
    wide_ref[pl.ds(inner_at, R)] = wide_ref[pl.ds(inner_at, R)] + inner_ref[...].astype(F32)
    wide_ref[pl.ds(outer_at, R)] = wide_ref[pl.ds(outer_at, R)] + outer_ref[...].astype(F32)
    standard, inv_std = normalize(grid_ref[...])
    scaled = wide_ref[...] * gain_ref[...]
    out_ref[...] = (
        inv_std
        * (
            scaled
            - jnp.mean(scaled, axis=-1, keepdims=True)
            - standard * jnp.mean(scaled * standard, axis=-1, keepdims=True)
        )
    ).astype(BF16)


def total_kernel(*refs):
    total = refs[0][...]
    for ref in refs[1:-1]:
        total = total + ref[...].astype(F32)
    refs[-1][...] = total


def swapped(value, band_bits, ens_bits):
    bands, members = lax.axis_size("band"), lax.axis_size("ens")
    flip = band_bits * members + ens_bits
    pairs = [(i, i ^ flip) for i in range(bands * members)]
    return lax.ppermute(value, ("band", "ens"), pairs)


def outward(value):
    bands = lax.axis_size("band")
    pairs = [(i, i + 1) for i in range(1, bands - 1, 2)]
    return lax.ppermute(value, "band", pairs + [(j, i) for i, j in pairs])


def beyond(value):
    bands = lax.axis_size("band")
    pairs = [(i, i + 2) for i in range(1, bands - 2, 2)]
    return lax.ppermute(value, "band", pairs + [(i + 2, i) for i in range(0, bands - 2, 2)])


def call(kernel, name, shapes, operands, scratch=(), flops=0, moved=0, **options):
    if "in_specs" not in options:
        options["in_specs"] = [spec()] * len(operands)
        options["out_specs"] = [spec()] * len(shapes)
    return pl.pallas_call(
        kernel,
        out_shape=[jax.ShapeDtypeStruct(*shape) for shape in shapes],
        scratch_shapes=[pltpu.VMEM(*shape) for shape in scratch],
        cost_estimate=estimate(flops, moved),
        compiler_params=pltpu.CompilerParams(vmem_limit_bytes=LIMIT),
        name=name,
        **options,
    )(*operands)


def per_device(grid_latent, hidden, d_updated, w_kv, w_q, src_gain, q_gain, src_index, edge_mask):
    grid_latent, hidden, d_updated = grid_latent[0], hidden[0], d_updated[0]
    rows, features = grid_latent.shape
    nodes = hidden.shape[0]
    bands, members = lax.axis_size("band"), lax.axis_size("ens")
    window = rows + 2 * R
    block = 2 * features // (bands * members)
    groups = bands // 2
    src_gain, q_gain = src_gain[None], q_gain[None]
    grouped = members == 4 and groups & (groups - 1) == 0 and block == features // HEADS == 64
    grouped = grouped and features == 8 * 128 and K * nodes + nodes <= features // 2
    square = features * features

    normed, edge = call(
        norm_kernel, "norm", [((rows, features), BF16), ((R, features), BF16)],
        [grid_latent, src_gain], flops=1e10, moved=4 * rows * features,
    )
    outer = outward(edge)
    pair = swapped(normed, 1, 0)
    if grouped:
        side = swapped(normed, 0, 2)
    far = beyond(edge)

    queries, kv = call(
        project_kernel, "project", [((nodes, features), BF16), ((rows, 2 * features), BF16)],
        [hidden, q_gain, w_q, normed, w_kv], flops=2 * (2 * rows + nodes) * square, moved=6 * square,
    )
    if grouped:
        side_pair = swapped(jnp.concatenate([pair, outer, far], axis=0), 0, 2)

    pieces = 1 if grouped else 0
    updated, partial_value, *lefts = call(
        attend_kernel, "attend",
        [((nodes, features), BF16), ((window, 2 * features), BF16)]
        + [((window, features // 2), BF16)] * pieces
        + [((SLOTS + nodes, features // 2), BF16)] * (3 * pieces),
        [outer, pair, w_kv, kv, queries, d_updated, hidden, src_index.T, edge_mask.T],
        [
            ((2 * R, features), BF16), ((2 * R, 2 * features), BF16),
            ((window, 2 * features), BF16),
        ],
        flops=3e9, moved=4 * square,
    )
    if grouped:
        lefts = [lefts[0], swapped(lefts[1], 0, 2), swapped(lefts[2], 1, 0), swapped(lefts[3], 1, 2)]

    d_own, d_inner, d_outer = call(
        window_kernel, "window",
        [((rows, features), F32), ((R, features), BF16), ((R, features), BF16)],
        [partial_value, w_kv], [((window, features), F32)],
        flops=4 * window * square, moved=4 * square,
    )
    d_inner = swapped(d_inner, 1, 0)
    d_outer = outward(d_outer)

    factor = 1.0 / math.sqrt(members * rows * bands)
    if grouped:
        *lefts, _ = lax.optimization_barrier((*lefts, d_own))
        operands = [*lefts, normed, outer, pair, far, side, side_pair]
        columns = features // 4
        buffers = [((4 * window, columns), BF16), ((4 * window, features), BF16)]
        (send,) = call(
            functools.partial(product_kernel, factor, 0), "product_send",
            [((columns, features), BF16)], operands, buffers,
            flops=2 * window * square, moved=4 * square,
        )
        got = swapped(send, 0, 1)
        (keep,) = call(
            functools.partial(product_kernel, factor, columns), "product_keep",
            [((columns, features), F32)], operands, buffers,
            flops=2 * window * square, moved=4 * square,
        )
        parts = call(
            pair_kernel, "pair",
            [((block, features), F32)] + [((block, features), BF16)] * (groups - 1),
            [keep, got], flops=square, moved=4 * square,
        )
        parts = [parts[0]] + [swapped(parts[k], 2 * k, 0) for k in range(1, groups)]
        (d_wkv_t,) = call(total_kernel, "total", [((block, features), F32)], parts)
    else:
        odd = lax.rem(lax.axis_index("band"), 2) == 1
        low = jnp.where(odd, pair[rows - R :], outer)
        high = jnp.where(odd, outer, pair[:R])
        normed_window = jnp.concatenate([low, normed, high], axis=0)
        d_wkv_t = lax.psum_scatter(
            dot_rows(partial_value, normed_window) * factor,
            ("band", "ens"), scatter_dimension=0, tiled=True,
        )

    (d_grid,) = call(
        finish_kernel, "finish", [((rows, features), BF16)],
        [grid_latent, src_gain, d_own, d_inner, d_outer], [((rows, features), F32)],
        flops=20 * rows * features, moved=8 * rows * features,
    )
    return (updated[None], d_grid[None], d_wkv_t)


def solution(mesh):
    return jax.shard_map(
        per_device,
        mesh=mesh,
        in_specs=(
            P("ens", "band", None),
            P("ens", "band", None),
            P("ens", "band", None),
            P(),
            P(),
            P(),
            P(),
            P("band", None),
            P("band", None),
        ),
        out_specs=(P("ens", "band", None), P("ens", "band", None), P(("band", "ens"), None)),
        check_vma=False,
    )
```

```python
import functools
import math

import jax
import jax.numpy as jnp
from jax import lax
from jax.experimental import pallas as pl
from jax.experimental.pallas import tpu as pltpu
from jax.sharding import PartitionSpec as P


HEADS = 16
K = 12
R = 32
EPSILON = 1e-05
SLOTS = 16
NOWHERE = 255
LIMIT = 24 << 20
F32 = jnp.float32
BF16 = jnp.bfloat16


def spec(space=pltpu.VMEM):
    return pl.BlockSpec(memory_space=space)


def estimate(flops, moved):
    return pl.CostEstimate(flops=int(flops), bytes_accessed=int(moved), transcendentals=0)


def dot(left, right):
    return jnp.dot(left, right, preferred_element_type=F32)


def dot_rows(left, right):
    return lax.dot_general(left, right, (((0,), (0,)), ((), ())), preferred_element_type=F32)


def dot_lanes(left, right):
    return lax.dot_general(left, right, (((1,), (1,)), ((), ())), preferred_element_type=F32)


def halves(wide):
    high = wide.astype(BF16)
    return high, (wide - high.astype(F32)).astype(BF16)


def normalize(values):
    values = values.astype(F32)
    average = jnp.mean(values, axis=-1, keepdims=True)
    centred = values - average
    variance = jnp.mean(centred * centred, axis=-1, keepdims=True)
    inv_std = lax.rsqrt(variance + EPSILON)
    return centred * inv_std, inv_std


def parity():
    return lax.rem(lax.axis_index("band"), 2)


def pick(flag, one, zero):
    return flag * one + (1 - flag) * zero


def early_kernel(out_ref):
    out_ref[...] = jnp.zeros_like(out_ref)


def norm_kernel(early_ref, grid_ref, gain_ref, normed_ref, edge_ref):
    standard, _ = normalize(grid_ref[...])
    normed_ref[...] = (standard * gain_ref[...]).astype(BF16)
    last = normed_ref.shape[0] - R
    odd = parity()
    edge_ref[...] = normed_ref[pl.ds(pl.multiple_of(pick(odd, last, 0), R), R)]


def slot_rows(index_ref, mask_ref, first_row):
    return jnp.where(mask_ref[...] > 0, index_ref[...] - first_row, NOWHERE).astype(F32).astype(BF16)


def counted(slots, nodes, rows):
    lanes = 128
    eye_a = lax.broadcasted_iota(jnp.int32, (slots.shape[0], lanes), 0)
    eye_b = lax.broadcasted_iota(jnp.int32, (slots.shape[0], lanes), 1)
    eye = jnp.where(eye_a == eye_b, 1.0, 0.0).astype(BF16)
    local = dot_rows(slots, eye)[:nodes].astype(jnp.int32)
    row_id = lax.broadcasted_iota(jnp.int32, (nodes, rows), 1)
    counts = jnp.zeros((nodes, rows), F32)
    for k in range(K):
        counts = counts + jnp.where(row_id == local[:, k : k + 1], 1.0, 0.0)
    return counts


def by_head(values, heads):
    nodes, columns = values.shape
    lane_head = lax.broadcasted_iota(jnp.int32, (nodes, columns), 1) // (columns // heads)
    wide = values.astype(F32)
    return jnp.concatenate(
        [jnp.where(lane_head == n, wide, 0.0).astype(BF16) for n in range(heads)], axis=0
    )


def twice(first, second):
    return jnp.concatenate([first, second], axis=0)


def attended_blocks(sources, heads, full):
    keys, values, queries, cotangents, counts = zip(*sources)
    columns, nodes = keys[0].shape[1], counts[0].shape[0]
    scale = 1.0 / math.sqrt(columns // heads)
    queries = [by_head(value, heads) for value in queries]
    cotangents = [by_head(value, heads) for value in cotangents]
    counts = jnp.concatenate([value for value in counts for _ in range(heads)], axis=0)
    scores = jnp.concatenate([dot_lanes(*pair) for pair in zip(queries, keys)], axis=0)
    d_probs = jnp.concatenate([dot_lanes(*pair) for pair in zip(cotangents, values)], axis=0)
    scores = jnp.where(counts > 0.0, scores * scale, -jnp.inf)
    terms = jnp.exp(scores - jnp.max(scores, axis=-1, keepdims=True))
    probs = terms / jnp.sum(counts * terms, axis=-1, keepdims=True)
    inner = jnp.sum(counts * probs * d_probs, axis=-1, keepdims=True)
    p_first, p_second = halves(counts * probs.astype(BF16).astype(F32))
    d_first, d_second = halves(counts * (probs * (d_probs - inner) * scale))
    lane_head = lax.broadcasted_iota(jnp.int32, (nodes, columns), 1) // (columns // heads)
    results = []
    for i in range(len(sources)):
        rows = slice(i * heads * nodes, (i + 1) * heads * nodes)
        d_values = dot_rows(twice(p_first[rows], p_second[rows]), twice(cotangents[i], cotangents[i]))
        d_keys = dot_rows(twice(d_first[rows], d_second[rows]), twice(queries[i], queries[i]))
        attended = None
        if full:
            spread = dot(p_first[rows], values[i]) + dot(p_second[rows], values[i])
            attended = jnp.zeros((nodes, columns), F32)
            for n in range(heads):
                piece = spread[n * nodes : (n + 1) * nodes]
                attended = attended + jnp.where(lane_head == n, piece, 0.0)
        results.append((d_keys.astype(BF16), d_values.astype(BF16), attended))
    return results


def by_core(one, two, out_ref, row, at, core):
    count, lanes = one.shape
    half = lanes // 2
    one, two = one.astype(F32), two.astype(F32)
    left = lax.broadcasted_iota(jnp.int32, (count, lanes), 1) < half
    firsts = jnp.where(left, one, pltpu.roll(two, half, 1)).astype(BF16)
    seconds = jnp.where(left, pltpu.roll(one, half, 1), two).astype(BF16)
    first_at = pl.multiple_of((pick(core, 0, 2) + at) * lanes, lanes)
    second_at = pl.multiple_of((pick(core, 2, 0) + at) * lanes, lanes)
    out_ref[row : row + count, pl.ds(first_at, lanes)] = firsts
    out_ref[row : row + count, pl.ds(second_at, lanes)] = seconds


def group_index():
    return 2 * parity() + lax.axis_index("ens") // 2


def tile(start):
    return pl.ds(pl.multiple_of(start * 128, 128), 128)


def project_kernel(
    hidden_ref, gain_ref, wq_ref, normed_ref, wkv_ref, cot_ref, index_ref, mask_ref, q_ref, kv_ref,
    *packet_refs
):
    standard, _ = normalize(hidden_ref[...])
    hat = (standard * gain_ref[...]).astype(BF16)
    q_ref[...] = dot(hat, wq_ref[...]).astype(BF16)
    kv_ref[...] = dot(normed_ref[...], wkv_ref[...]).astype(BF16)
    nodes = q_ref.shape[0]
    first_row = lax.axis_index("band") * normed_ref.shape[0] - R
    for k, packet_ref in enumerate(packet_refs):
        group = group_index() ^ (k + 1)
        packet_ref[:SLOTS] = jnp.full((SLOTS, packet_ref.shape[1]), NOWHERE, BF16)
        packet_ref[:K, :nodes] = slot_rows(index_ref, mask_ref, first_row)
        for i in range(2):
            packet_ref[SLOTS:, i * 128 : (i + 1) * 128] = q_ref[:, tile(4 * i + group)]
            packet_ref[SLOTS:, (2 + i) * 128 : (3 + i) * 128] = cot_ref[:, tile(4 * i + group)]


def attend_kernel(
    outer_ref, pair_ref, gain_ref, wkv_ref, kv_ref, q_ref, cot_ref, hidden_ref, index_ref,
    mask_ref, updated_ref, partial_ref, beside_ref, d_outer_ref, *refs
):
    piece_refs, (both_ref, window_ref) = refs[:-2], refs[-2:]
    standard, _ = normalize(pair_ref[...])
    beside_ref[...] = (standard * gain_ref[...]).astype(BF16)
    nodes, features = q_ref.shape
    own = kv_ref.shape[0]
    rows = own + 2 * R
    odd = parity()
    outer_at = pl.multiple_of(pick(odd, R, 0), R)
    inner_at = pl.multiple_of(pick(odd, 0, R), R)
    from_at = pl.multiple_of(pick(odd, own - R, 0), R)
    both_ref[pl.ds(outer_at, R)] = outer_ref[...]
    both_ref[pl.ds(inner_at, R)] = beside_ref[pl.ds(from_at, R)]
    halo = dot(both_ref[...], wkv_ref[...]).astype(BF16)
    window_ref[:R] = halo[:R]
    window_ref[R : R + own] = kv_ref[...]
    window_ref[R + own :] = halo[R:]
    counts = counted(slot_rows(index_ref, mask_ref, lax.axis_index("band") * own - R), nodes, rows)
    heads = 4
    chunk = features // HEADS * heads
    starts = range(0, features, chunk)
    sources = [
        (
            window_ref[:, c : c + chunk],
            window_ref[:, features + c : features + c + chunk],
            q_ref[:, c : c + chunk],
            cot_ref[:, c : c + chunk],
            counts,
        )
        for c in starts
    ]
    for c, (d_keys, d_values, attended) in zip(starts, attended_blocks(sources, heads, True)):
        partial_ref[:, c : c + chunk] = d_keys
        partial_ref[:, features + c : features + c + chunk] = d_values
        updated_ref[:, c : c + chunk] = (
            hidden_ref[:, c : c + chunk].astype(F32) + attended
        ).astype(BF16)
    last = pl.multiple_of(pick(odd, rows - R, 0), R)
    d_outer_ref[...] = dot_lanes(partial_ref[pl.ds(last, R)], wkv_ref[...]).astype(BF16)
    core = lax.rem(lax.axis_index("ens"), 2)
    for piece_ref in piece_refs:
        for i in range(2):
            one, two = (partial_ref[:, tile(4 * t + group_index())] for t in (2 * i, 2 * i + 1))
            by_core(one, two, piece_ref, 0, i, core)


def window_kernel(partial_ref, wkv_ref, own_ref, inner_ref, wide_ref):
    wide_ref[...] = dot_lanes(partial_ref[...], wkv_ref[...])
    rows = wide_ref.shape[0]
    odd = parity()
    inner_at = pl.multiple_of(pick(odd, 0, rows - R), R)
    own_ref[...] = wide_ref[R : rows - R]
    inner_ref[...] = wide_ref[pl.ds(inner_at, R)].astype(BF16)


def rebuild_kernel(*refs):
    piece_ref, packets, (own, outer, pair, side, rest_ref) = refs[0], refs[1:4], refs[4:9]
    gain_ref, wkv_ref, left_ref, right_ref, columns_ref, kv_ref, rest = refs[9:]
    window, rows = piece_ref.shape[0], own.shape[0]
    nodes, half = packets[0].shape[0] - SLOTS, columns_ref.shape[1] // 2
    pack = slice(SLOTS, SLOTS + nodes)
    odd = parity()
    core = lax.rem(lax.axis_index("ens"), 2)
    left_ref[:window] = piece_ref[...]
    standard, _ = normalize(rest_ref[:rows])
    rest[:rows] = (standard * gain_ref[...]).astype(BF16)
    rest[rows:] = rest_ref[rows:]
    pieces = (
        ((own, 0), (outer, 0), (pair, 0)),
        ((side, 0), (rest, rows), (rest, 0)),
        ((pair, 0), (packets[1], SLOTS + nodes), (own, 0)),
        ((rest, 0), (packets[2], SLOTS + nodes), (side, 0)),
    )
    for k, ((middle, m_at), (edge, e_at), (other, o_at)) in enumerate(pieces):
        base = k * window
        right_ref[base + R : base + R + rows] = middle[m_at : m_at + rows]
        flag = odd if k < 2 else 1 - odd
        edge_at = pl.multiple_of(base + pick(flag, R + rows, 0), R)
        other_at = pl.multiple_of(base + pick(flag, 0, R + rows), R)
        from_at = pl.multiple_of(o_at + pick(flag, rows - R, 0), R)
        wide = edge.shape[1]
        for i in range(right_ref.shape[1] // wide):
            rows_at = slice(e_at + i * R, e_at + (i + 1) * R)
            right_ref[pl.ds(edge_at, R), i * wide : (i + 1) * wide] = edge[rows_at]
        right_ref[pl.ds(other_at, R)] = other[pl.ds(from_at, R)]
    for i in range(4):
        columns_ref[:, i * 128 : (i + 1) * 128] = wkv_ref[:, tile(4 * i + group_index())]
    kv_ref[...] = dot(right_ref[window:], columns_ref[...]).astype(BF16)
    sources = []
    for k, packet in enumerate(packets):
        if k < 2:
            counts = counted(packet[:SLOTS, :128], nodes, window)
        source = slice(k * window, (k + 1) * window)
        sources.append(
            (
                kv_ref[source, :half], kv_ref[source, half:], packet[pack, :half],
                packet[pack, half:], counts,
            )
        )
    for k, parts in enumerate(attended_blocks(sources, 4, False)):
        for i, values in enumerate(parts[:2]):
            by_core(values[:, :128], values[:, 128:], left_ref, (k + 1) * window, i, core)


def product_kernel(factor, left_ref, right_ref, out_ref, *, start):
    columns = out_ref.shape[0]
    total = dot_rows(left_ref[:, start : start + columns], right_ref[...]) * factor
    out_ref[...] = total.astype(out_ref.dtype)


def pair_kernel(keep_ref, got_ref, *out_refs):
    group = lax.axis_index("band") // 2
    block = out_refs[0].shape[0]
    for k, out_ref in enumerate(out_refs):
        at = pl.ds(pl.multiple_of((group ^ k) * block, block), block)
        out_ref[...] = (keep_ref[at] + got_ref[at].astype(F32)).astype(out_ref.dtype)


def finish_kernel(grid_ref, gain_ref, own_ref, inner_ref, outer_ref, out_ref, wide_ref):
    rows = own_ref.shape[0]
    odd = parity()
    wide_ref[...] = own_ref[...]
    inner_at = pl.multiple_of(pick(odd, 0, rows - R), R)
    outer_at = pl.multiple_of(pick(odd, rows - R, 0), R)
    wide_ref[pl.ds(inner_at, R)] = wide_ref[pl.ds(inner_at, R)] + inner_ref[...].astype(F32)
    wide_ref[pl.ds(outer_at, R)] = wide_ref[pl.ds(outer_at, R)] + outer_ref[...].astype(F32)
    standard, inv_std = normalize(grid_ref[...])
    scaled = wide_ref[...] * gain_ref[...]
    out_ref[...] = (
        inv_std
        * (
            scaled
            - jnp.mean(scaled, axis=-1, keepdims=True)
            - standard * jnp.mean(scaled * standard, axis=-1, keepdims=True)
        )
    ).astype(BF16)


def total_kernel(*refs):
    total = refs[0][...]
    for ref in refs[1:-1]:
        total = total + ref[...].astype(F32)
    refs[-1][...] = total


def swapped(value, band_bits, ens_bits):
    bands, members = lax.axis_size("band"), lax.axis_size("ens")
    flip = band_bits * members + ens_bits
    pairs = [(i, i ^ flip) for i in range(bands * members)]
    return lax.ppermute(value, ("band", "ens"), pairs)


def outward(value):
    bands = lax.axis_size("band")
    pairs = [(i, i + 1) for i in range(1, bands - 1, 2)]
    return lax.ppermute(value, "band", pairs + [(j, i) for i, j in pairs])


def call(kernel, shapes, operands, scratch=(), flops=0, moved=0, **options):
    if "in_specs" not in options:
        options["in_specs"] = [spec()] * len(operands)
        options["out_specs"] = [spec()] * len(shapes)
    return pl.pallas_call(
        kernel,
        out_shape=[jax.ShapeDtypeStruct(*shape) for shape in shapes],
        scratch_shapes=[pltpu.VMEM(*shape) for shape in scratch],
        cost_estimate=estimate(flops, moved),
        compiler_params=pltpu.CompilerParams(vmem_limit_bytes=LIMIT),
        **options,
    )(*operands)


def per_device(grid_latent, hidden, d_updated, w_kv, w_q, src_gain, q_gain, src_index, edge_mask):
    grid_latent, hidden, d_updated = grid_latent[0], hidden[0], d_updated[0]
    rows, features = grid_latent.shape
    nodes = hidden.shape[0]
    bands, members = lax.axis_size("band"), lax.axis_size("ens")
    window = rows + 2 * R
    block = 2 * features // (bands * members)
    groups = bands // 2
    src_gain, q_gain = src_gain[None], q_gain[None]
    grouped = members == 4 and groups & (groups - 1) == 0 and block == features // HEADS == 64
    grouped = grouped and features == 8 * 128 and K * nodes + nodes <= features // 2
    square = features * features

    (early,) = call(early_kernel, [((8, 128), F32)], [], flops=1e10)
    normed, edge = call(
        norm_kernel, [((rows, features), BF16), ((R, features), BF16)],
        [early, grid_latent, src_gain], flops=1e6, moved=4 * rows * features,
    )
    outer = outward(edge)
    pair = swapped(grid_latent, 1, 0)
    if grouped:
        side = swapped(normed, 0, 2)
        rest = swapped(jnp.concatenate([pair, outer], axis=0), 0, 2)
        wide = features // 2
        halo = [outer[:, :wide], outer[:, wide:]]

    pieces = 1 if grouped else 0
    index, mask = src_index.T, edge_mask.T
    queries, kv, *packets = call(
        project_kernel,
        [((nodes, features), BF16), ((rows, 2 * features), BF16)]
        + [((SLOTS + nodes, features // 2), BF16)] * (3 * pieces),
        [hidden, q_gain, w_q, normed, w_kv, d_updated, index, mask],
        flops=2 * (2 * rows + nodes) * square, moved=6 * square,
    )
    if grouped:
        packets = [
            swapped(packets[0], 0, 2),
            swapped(jnp.concatenate([packets[1], *halo], axis=0), 1, 0),
            swapped(jnp.concatenate([packets[2], *halo], axis=0), 1, 2),
        ]
    updated, partial_value, beside, d_outer, *piece = call(
        attend_kernel,
        [
            ((nodes, features), BF16), ((window, 2 * features), BF16),
            ((rows, features), BF16), ((R, features), BF16),
        ]
        + [((window, features // 2), BF16)] * pieces,
        [outer, pair, src_gain, w_kv, kv, queries, d_updated, hidden, index, mask],
        [((2 * R, features), BF16), ((window, 2 * features), BF16)],
        flops=3e9, moved=4 * square,
    )
    d_own, d_inner = call(
        window_kernel, [((rows, features), F32), ((R, features), BF16)],
        [partial_value, w_kv], [((window, features), F32)],
        flops=4 * window * square, moved=4 * square,
    )
    d_outer = outward(d_outer)
    d_inner = swapped(d_inner, 1, 0)

    factor = 1.0 / math.sqrt(members * rows * bands)
    if grouped:
        left, right = call(
            rebuild_kernel,
            [((4 * window, features // 2), BF16), ((4 * window, features), BF16)],
            [*piece, *packets, normed, outer, beside, side, rest, src_gain, w_kv],
            [
                ((features, features // 2), BF16), ((3 * window, features // 2), BF16),
                ((rows + R, features), BF16),
            ],
            flops=6 * window * square, moved=4 * square,
        )
        columns = features // 4
        (send,) = call(
            functools.partial(product_kernel, factor, start=0),
            [((columns, features), BF16)], [left, right],
            flops=2 * window * square, moved=4 * square,
        )
        got = swapped(send, 0, 1)
        (keep,) = call(
            functools.partial(product_kernel, factor, start=columns),
            [((columns, features), F32)], [left, right],
            flops=2 * window * square, moved=4 * square,
        )
        parts = call(
            pair_kernel,
            [((block, features), F32)] + [((block, features), BF16)] * (groups - 1),
            [keep, got], flops=square, moved=4 * square,
        )
        parts = [parts[0]] + [swapped(parts[k], 2 * k, 0) for k in range(1, groups)]
        (d_wkv_t,) = call(total_kernel, [((block, features), F32)], parts)
    else:
        odd = lax.rem(lax.axis_index("band"), 2) == 1
        low = jnp.where(odd, beside[rows - R :], outer)
        high = jnp.where(odd, outer, beside[:R])
        normed_window = jnp.concatenate([low, normed, high], axis=0)
        d_wkv_t = lax.psum_scatter(
            dot_rows(partial_value, normed_window) * factor,
            ("band", "ens"), scatter_dimension=0, tiled=True,
        )

    (d_grid,) = call(
        finish_kernel, [((rows, features), BF16)],
        [grid_latent, src_gain, d_own, d_inner, d_outer], [((rows, features), F32)],
        flops=20 * rows * features, moved=8 * rows * features,
    )
    return (updated[None], d_grid[None], d_wkv_t)


def solution(mesh):
    return sharded(mesh)


def sharded(mesh):
    return jax.shard_map(
        per_device,
        mesh=mesh,
        in_specs=(
            P("ens", "band", None),
            P("ens", "band", None),
            P("ens", "band", None),
            P(),
            P(),
            P(),
            P(),
            P("band", None),
            P("band", None),
        ),
        out_specs=(P("ens", "band", None), P("ens", "band", None), P(("band", "ens"), None)),
        check_vma=False,
    )
```
